16 devices in a mesh: dp: 4 (over y, z, core), tp: 4 (over x).
Axes of the slice: x: 4, y: 2, z: 1, core: 2. Of those that a mesh axis runs over, the one named last changes fastest.
The devices are a block of a 4x4x8 slice.
Arguments:
- x: bfloat16 [4, 1536, 3072], P('dp', 'tp'), parts along dimension 0
- dy: bfloat16 [4, 1536, 3072], P('dp', 'tp'), parts along dimension 0
- wq: bfloat16 [3072, 3072], P(None, 'tp')
- wk: bfloat16 [3072, 1024], P(None, 'tp')
- wv: bfloat16 [3072, 1024], P(None, 'tp')
- wo: bfloat16 [3072, 3072], P('tp')
- w_gate: bfloat16 [3072, 8192], P(None, 'tp')
- w_up: bfloat16 [3072, 8192], P(None, 'tp')
- w_down: bfloat16 [8192, 3072], P('tp')
Outputs:
- output 1: bfloat16 [4, 1536, 3072], P('dp', 'tp'), parts along dimension 0
- output 2: bfloat16 [12288, 3072], P('dp', 'tp'), parts along dimension 0
- output 3: bfloat16 [12288, 1024], P('dp', 'tp'), parts along dimension 0
- output 4: bfloat16 [12288, 1024], P('dp', 'tp'), parts along dimension 0
- output 5: bfloat16 [12288, 3072], P(('dp', 'tp')), parts along dimension 0
- output 6: bfloat16 [12288, 8192], P('dp', 'tp'), parts along dimension 0
- output 7: bfloat16 [12288, 8192], P('dp', 'tp'), parts along dimension 0
- output 8: bfloat16 [32768, 3072], P(('dp', 'tp')), parts along dimension 0
There are 4 independent parts. The reference program is written for one: setup_inputs(seed, part) draws one part's arguments, and reference() takes and returns one part's arrays. A program takes and returns all parts, laid end to end along the dimension named above; an argument that names none is the same for every part.
All inputs are finite; a program needn't handle non-finite values.
Results may differ from the reference program's by a relative error of at most 0.024.
Values are sent between devices in bfloat16 or wider.
A program may use at most 768 MiB of HBM per device.

```python
import jax
import jax.numpy as jnp
from jax import lax

SEQUENCES = 1
TOKENS = 1536
D = 3072
HEADS = 24
KV_HEADS = 8
HEAD = 128
FF = 8192
THETA = 10000
NAMES = ("wq", "wk", "wv", "wo", "w_gate", "w_up", "w_down")
SHAPES = {
    "wq": (D, HEADS * HEAD),
    "wk": (D, KV_HEADS * HEAD),
    "wv": (D, KV_HEADS * HEAD),
    "wo": (HEADS * HEAD, D),
    "w_gate": (D, FF),
    "w_up": (D, FF),
    "w_down": (FF, D),
}


def bump(key, n, height):
    away = (jnp.arange(n, dtype=jnp.int32) - jax.random.randint(key, (), 0, n, jnp.int32)) % n
    return jnp.where(away < n // 8, height, 1.0)


def together(key, own, strength):
    shared = jax.random.normal(key, own.shape[1:], jnp.float32)
    return (own + strength * shared) * lax.rsqrt(1 + strength * strength)


def setup_inputs(seed: int = 0, part: int = 0) -> dict:
    kx, kdy, ka, kb, kz, kf, kh, kl, *kw = jax.random.split(jax.random.key(seed), 8 + len(NAMES))
    kx, kdy, ka, kb = (jax.random.fold_in(k, part) for k in (kx, kdy, ka, kb))
    shape = (SEQUENCES, TOKENS, D)
    much_x, much_dy = jax.random.uniform(kz, (2,), jnp.float32, 0.0, 1.0)
    loud = 2.0 ** jax.random.uniform(jax.random.fold_in(kz, 1), (), jnp.float32, -1.0, 2.0)
    halves = 2.0 ** jax.random.uniform(kl, (2,), jnp.float32, -1.0, 1.0)
    times = {"wq": 1.0, "wk": 1.0, "wv": 2.0, "wo": halves[0], "w_gate": 1.0, "w_up": bump(kh, FF, 4.0), "w_down": halves[1]}
    x = together(ka, jax.random.normal(kx, shape, jnp.float32), much_x) * bump(kf, D, 4.0)
    dy = together(kb, jax.random.normal(kdy, shape, jnp.float32), much_dy)
    drawn = {"x": x.astype(jnp.bfloat16), "dy": (loud * dy * (SEQUENCES * TOKENS) ** -0.5).astype(jnp.bfloat16)}
    for key, name in zip(kw, NAMES, strict=True):
        drawn[name] = (jax.random.normal(key, SHAPES[name], jnp.float32) * SHAPES[name][0] ** -0.5 * times[name]).astype(jnp.bfloat16)
    return drawn


def matmul(a, w):
    return jnp.dot(a, w, preferred_element_type=jnp.float32).astype(jnp.bfloat16)


def normed(h):
    wide = h.astype(jnp.float32)
    scale = lax.rsqrt(jnp.mean(wide**2, -1, keepdims=True) + 1e-6)
    return (wide * scale).astype(jnp.bfloat16)


def turned(t, theta):
    half = t.shape[-1] // 2
    angle = jnp.arange(t.shape[0], dtype=jnp.float32)[:, None] * theta ** (-jnp.arange(half, dtype=jnp.float32) / half)
    cos, sin = jnp.cos(angle)[:, None], jnp.sin(angle)[:, None]
    a, b = t[..., :half].astype(jnp.float32), t[..., half:].astype(jnp.float32)
    return jnp.concatenate([a * cos - b * sin, b * cos + a * sin], -1).astype(jnp.bfloat16)


def seen_by(q, k, v):
    tokens, kv = q.shape[0], k.shape[1]
    q = q.reshape(tokens, kv, -1, q.shape[-1])
    scores = jnp.einsum("tgsd,ugd->gstu", q.astype(jnp.float32), k.astype(jnp.float32)) * q.shape[-1] ** -0.5
    place = jnp.arange(tokens)
    weights = jax.nn.softmax(jnp.where(place[:, None] >= place, scores, -jnp.inf), -1).astype(jnp.bfloat16)
    return jnp.einsum("gstu,ugd->tgsd", weights.astype(jnp.float32), v.astype(jnp.float32)).astype(jnp.bfloat16).reshape(tokens, -1)


def layer(h, w):
    a = normed(h)
    q, k = (turned(matmul(a, w[name]).reshape(h.shape[0], -1, HEAD), THETA) for name in ("wq", "wk"))
    h = h + matmul(seen_by(q, k, matmul(a, w["wv"]).reshape(h.shape[0], -1, HEAD)), w["wo"])
    b = normed(h)
    gate = jnp.dot(b, w["w_gate"], preferred_element_type=jnp.float32)
    up = jnp.dot(b, w["w_up"], preferred_element_type=jnp.float32)
    return h + matmul((jax.nn.silu(gate) * up).astype(jnp.bfloat16), w["w_down"])


def reference(x, dy, wq, wk, wv, wo, w_gate, w_up, w_down):
    weights = dict(zip(NAMES, (wq, wk, wv, wo, w_gate, w_up, w_down), strict=True))

    def take(so_far, sequence):
        h, by_y = sequence
        _, back = jax.vjp(lambda w, h: layer(h, w), weights, h)
        by_weights, by_h = back(by_y)
        return jax.tree.map(lambda total, term: total + term.astype(jnp.float32), so_far, by_weights), by_h

    none_yet = {name: jnp.zeros(w.shape, jnp.float32) for name, w in weights.items()}
    by_weights, by_x = lax.scan(take, none_yet, (x, dy))
    return (by_x, *(by_weights[name].astype(jnp.bfloat16) for name in NAMES))
```

```python
import functools

import jax
import jax.numpy as jnp
from jax import lax
from jax.experimental import pallas as pl
from jax.experimental.pallas import tpu as pltpu

NEG = -1e30
HIDDEN = 2 * NEG
LOG2E = 1.4426950408889634
HEAD = 128


def _fit(size, want, unit=128):
    return max(n for n in range(unit, max(min(want, size), unit) + 1, unit) if size % n == 0)


def _dot(a, b, ca, cb):
    return lax.dot_general(a, b, (((ca,), (cb,)), ((), ())), preferred_element_type=jnp.float32)


def _turn(t, cos, sin, back=False):
    other = pltpu.roll(t, HEAD // 2, 1) * sin
    return t * cos - other if back else t * cos + other


def _blocks(iq, bq, bk, total):
    return lax.div(iq * bq + 1, bk), jnp.minimum(lax.div(iq * bq + bq - 1 + bk, bk), total)


def _gap(bk, bq):
    return lax.broadcasted_iota(jnp.int32, (bk, bq), 1) - lax.broadcasted_iota(jnp.int32, (bk, bq), 0)


def _cols(n):
    return slice(n * HEAD, (n + 1) * HEAD)


def _turn_keys(k_ref, cos_ref, sin_ref, k_s):
    step = 256

    @pl.loop(0, k_ref.shape[0] // step)
    def _(i):
        r = pl.ds(pl.multiple_of(i * step, step), step)
        for n in range(k_ref.shape[1] // HEAD):
            k_s[r, _cols(n)] = _turn(k_ref[r, _cols(n)].astype(jnp.float32), cos_ref[r, :], sin_ref[r, :]).astype(k_s.dtype)


def _turn_queries(iq, q_ref, cos_ref, sin_ref, q_s):
    bq = q_ref.shape[0]
    here = pl.ds(pl.multiple_of(iq * bq, bq), bq)
    for n in range(q_ref.shape[1] // HEAD):
        q_s[:, _cols(n)] = _turn(q_ref[:, _cols(n)].astype(jnp.float32), cos_ref[here, :], sin_ref[here, :]).astype(q_s.dtype)


def _forward(q_ref, k_ref, v_ref, cos_ref, sin_ref, o_ref, lse_ref, q_s, k_s, top_s, mix_s, gap_s, *, bk):
    bq, heads, kv = q_ref.shape[0], q_ref.shape[1] // HEAD, k_ref.shape[1] // HEAD
    g, scale = heads // kv, HEAD**-0.5
    e, low = scale * LOG2E, q_ref.dtype
    iq = pl.program_id(0)

    @pl.when(iq == 0)
    def _():
        gap_s[...] = _gap(bk, bq)
        _turn_keys(k_ref, cos_ref, sin_ref, k_s)

    _turn_queries(iq, q_ref, cos_ref, sin_ref, q_s)
    top_s[...] = jnp.full_like(top_s, NEG)
    mix_s[...] = jnp.zeros_like(mix_s)
    ones = jnp.ones((8, bk), low)

    def block(j, masked):
        here = pl.ds(pl.multiple_of(j * bk, bk), bk)
        scores = [_dot(k_s[here, _cols(n // g)], q_s[:, _cols(n)], 1, 1) for n in range(heads)]
        ok = gap_s[...] >= j * bk - iq * bq if masked else None
        weights, keeps = [], []
        for n, s in enumerate(scores):
            if masked:
                s = jnp.where(ok, s, HIDDEN)
            old = top_s[n : n + 1, :]
            top = jnp.maximum(old, s.max(axis=0, keepdims=True))
            top_s[n : n + 1, :] = top
            weights.append(jnp.exp2((s - top) * e).astype(low))
            keeps.append(jnp.exp2((old - top) * e))
        for n, (p, keep) in enumerate(zip(weights, keeps)):
            values = jnp.concatenate([v_ref[here, _cols(n // g)].T, ones], axis=0)
            mix_s[n] = mix_s[n] * keep + _dot(values, p, 1, 0)

    whole, last = _blocks(iq, bq, bk, k_ref.shape[0] // bk)
    lax.fori_loop(0, whole, lambda j, _: block(j, False), None)
    lax.fori_loop(whole, last, lambda j, _: block(j, True), None)
    for n in range(heads):
        total = mix_s[n, HEAD : HEAD + 1, :]
        o_ref[:, _cols(n)] = (mix_s[n, :HEAD, :] * (1 / total)).T.astype(o_ref.dtype)
        lse_ref[n : n + 1, :] = top_s[n : n + 1, :] * scale + jnp.log(total)


def _backward(q_ref, k_ref, v_ref, cos_ref, sin_ref, do_ref, o_ref, lse_ref, *rest, bk, moved):
    given, rest = rest[:moved], rest[moved:]
    dq_ref, dk_ref, dv_ref = rest[:3]
    taken, (q_s, k_s, dq_s, dk_s, dv_s, gap_s) = rest[3 : 3 + moved], rest[3 + moved :]
    bq, heads, kv = q_ref.shape[0], q_ref.shape[1] // HEAD, k_ref.shape[1] // HEAD
    g, scale = heads // kv, HEAD**-0.5
    e, low = scale * LOG2E, q_ref.dtype
    iq = pl.program_id(0)

    @pl.when(iq == 0)
    def _():
        gap_s[...] = _gap(bk, bq)
        _turn_keys(k_ref, cos_ref, sin_ref, k_s)
        dk_s[...] = jnp.zeros_like(dk_s)
        dv_s[...] = jnp.zeros_like(dv_s)

    _turn_queries(iq, q_ref, cos_ref, sin_ref, q_s)
    dq_s[...] = jnp.zeros_like(dq_s)
    for source, target in zip(given, taken):
        target[...] = source[...]
    lses, deltas = [], []
    for n in range(heads):
        both = do_ref[:, _cols(n)].astype(jnp.float32) * o_ref[:, _cols(n)].astype(jnp.float32)
        deltas.append(both.T.sum(axis=0, keepdims=True))
        lses.append(lse_ref[n : n + 1, :] * LOG2E)

    def block(j, masked):
        here = pl.ds(pl.multiple_of(j * bk, bk), bk)
        scores = [_dot(k_s[here, _cols(n // g)], q_s[:, _cols(n)], 1, 1) for n in range(heads)]
        dps = [_dot(v_ref[here, _cols(n // g)], do_ref[:, _cols(n)], 1, 1) for n in range(heads)]
        ok = gap_s[...] >= j * bk - iq * bq if masked else None
        for n in range(heads):
            p = jnp.exp2(scores[n] * e - lses[n])
            if masked:
                p = jnp.where(ok, p, 0.0)
            ds = (p * (dps[n] - deltas[n])).astype(low)
            c = _cols(n // g)
            dv_s[here, c] += _dot(p.astype(low), do_ref[:, _cols(n)], 1, 0)
            dk_s[here, c] += _dot(ds, q_s[:, _cols(n)], 1, 0)
            dq_s[n] += _dot(k_s[here, c].T, ds, 1, 0)

    whole, last = _blocks(iq, bq, bk, k_ref.shape[0] // bk)
    lax.fori_loop(0, whole, lambda j, _: block(j, False), None)
    lax.fori_loop(whole, last, lambda j, _: block(j, True), None)
    mine = pl.ds(pl.multiple_of(iq * bq, bq), bq)
    for n in range(heads):
        dq_ref[:, _cols(n)] = _turn((dq_s[n] * scale).T, cos_ref[mine, :], sin_ref[mine, :], True).astype(dq_ref.dtype)

    @pl.when(iq == pl.num_programs(0) - 1)
    def _():
        step = 256

        @pl.loop(0, dk_s.shape[0] // step)
        def _(i):
            r = pl.ds(pl.multiple_of(i * step, step), step)
            dv_ref[r, :] = dv_s[r, :].astype(dv_ref.dtype)
            for n in range(kv):
                dk_ref[r, _cols(n)] = _turn(dk_s[r, _cols(n)] * scale, cos_ref[r, :], sin_ref[r, :], True).astype(dk_ref.dtype)


def _views(qkv, width, kv_width, bq):
    tokens = qkv.shape[0]
    at = width // kv_width
    return [pl.BlockSpec((bq, width), lambda i: (i, 0)), pl.BlockSpec((tokens, kv_width), lambda i: (0, at)), pl.BlockSpec((tokens, kv_width), lambda i: (0, at + 1))]


def attention_back(qkv, cos, sin, d_out, out, lse, kv_width, pass_on, *, bq=256, bk=384):
    tokens, width = d_out.shape
    heads = width // HEAD
    bq, bk = _fit(tokens, bq), _fit(tokens, bk)
    steps = tokens // bq
    mine = pl.BlockSpec((bq, width), lambda i: (i, 0))
    table = pl.BlockSpec((tokens, HEAD), lambda i: (0, 0))
    keys = pl.BlockSpec((tokens, kv_width), lambda i: (0, 0))
    runs = [pl.BlockSpec((t.shape[0] // steps, t.shape[1]), lambda i: (i, 0)) if t.shape[0] % (16 * steps) == 0 else pl.BlockSpec((t.shape[0], t.shape[1] // steps), lambda i: (0, i))
            for t in pass_on]
    low = qkv.dtype
    return pl.pallas_call(
        functools.partial(_backward, bk=bk, moved=len(pass_on)), name="attention_back", grid=(steps,),
        in_specs=[*_views(qkv, width, kv_width, bq), table, table, mine, mine, pl.BlockSpec((heads, bq), lambda i: (0, i)), *runs],
        out_specs=[mine, keys, keys, *runs],
        out_shape=[jax.ShapeDtypeStruct((tokens, width), low), jax.ShapeDtypeStruct((tokens, kv_width), low), jax.ShapeDtypeStruct((tokens, kv_width), low),
                   *(jax.ShapeDtypeStruct(t.shape, t.dtype) for t in pass_on)],
        scratch_shapes=[pltpu.VMEM((bq, width), low), pltpu.VMEM((tokens, kv_width), low), pltpu.VMEM((heads, HEAD, bq), jnp.float32),
                        pltpu.VMEM((tokens, kv_width), jnp.float32), pltpu.VMEM((tokens, kv_width), jnp.float32), pltpu.VMEM((bk, bq), jnp.int32)],
        compiler_params=pltpu.CompilerParams(dimension_semantics=("arbitrary",), vmem_limit_bytes=60 * 2**20),
        cost_estimate=pl.CostEstimate(flops=10 * heads * tokens * tokens * HEAD, transcendentals=heads * tokens * tokens, bytes_accessed=8 * tokens * width),
    )(qkv, qkv, qkv, cos, sin, d_out, out, lse, *pass_on)

from jax.sharding import PartitionSpec as P

THETA = 10000
BF16, F32 = jnp.bfloat16, jnp.float32
MESH = pl.DeviceIdType.MESH
ANY = pl.BlockSpec(memory_space=pl.ANY)


def norm_scale(wide):
    return lax.rsqrt(jnp.mean(wide**2, -1, keepdims=True) + 1e-6)


def normed(wide):
    return (wide * norm_scale(wide)).astype(BF16)


def norm_back(wide, by_out):
    scale = norm_scale(wide)
    along = jnp.mean(wide * by_out, -1, keepdims=True)
    return scale * by_out - wide * (along * scale**3)


def tables(tokens):
    half = HEAD // 2
    angle = jnp.arange(tokens, dtype=F32)[:, None] * THETA ** (-(jnp.arange(HEAD) % half).astype(F32) / half)
    return jnp.cos(angle), jnp.sin(angle) * jnp.where(jnp.arange(HEAD) < half, -1.0, 1.0)


class Ring:
    def __init__(self, n, rows):
        self.n, self.rows, self.half = n, rows, rows // 2
        self.me = lax.axis_index("tp")
        self.right, self.left = lax.rem(self.me + 1, n), lax.rem(self.me + n - 1, n)
        self.across = lax.rem(self.me + 2, n)

    def greet(self):
        barrier = pltpu.get_barrier_semaphore()
        for to in (self.left, self.right):
            pl.semaphore_signal(barrier, inc=1, device_id={"tp": to}, device_id_type=MESH)
        pl.semaphore_wait(barrier, 2)

    def copy(self, src, dst, send, recv, to):
        return pltpu.make_async_remote_copy(src_ref=src, dst_ref=dst, send_sem=send, recv_sem=recv, device_id={"tp": to}, device_id_type=MESH)

    def push(self, *where):
        copy = self.copy(*where)
        copy.start()
        return copy

    def places(self, group):
        rows, half = self.rows, self.half
        return {
            "O": (self.me * rows, self.me * rows + half),
            "X": (self.left * rows, self.right * rows + half),
            "Y": (self.left * rows + half, self.right * rows),
            "Z": (self.across * rows, self.across * rows + half),
        }[group]


class Gather:
    def __init__(self, ring, own, at, send, recv, first=None):
        self.ring, self.own, self.send, self.recv, self.copies = ring, own, send, recv, {}
        self.at = dict(at, O=own) if first is None else dict(at, O=own, X=first)

    def step(self, group):
        r, h = self.ring, self.ring.half
        top, bottom = pl.ds(0, h), pl.ds(h, h)
        k = 2 * "XYZ".index(group)
        source = self.at["X" if group == "Z" else "O"]
        right, left = (bottom, top) if group == "Y" else (top, bottom)
        self.copies[group] = (
            r.push(source.at[right], self.at[group].at[top], self.send.at[k], self.recv.at[k], r.right),
            r.push(source.at[left], self.at[group].at[bottom], self.send.at[k + 1], self.recv.at[k + 1], r.left),
        )

    def arrived(self, group):
        for copy in self.copies[group]:
            copy.wait_recv()

    def finish(self):
        for pair in self.copies.values():
            for copy in pair:
                copy.wait_send()

    def rows_of(self, group):
        return self.at[group]


def parts(ref, rows, groups):
    return {group: ref.at[pl.ds(i * rows, rows)] for i, group in enumerate(groups)}


class Scatter:
    def __init__(self, ring, out_s, in_s, send, recv):
        self.ring, self.out, self.inn, self.send, self.recv, self.copies = ring, out_s, in_s, send, recv, {}

    def step(self, group):
        r, h = self.ring, self.ring.half
        k = "XZY".index(group)
        first, second = pl.ds(0, h), pl.ds(h, h)
        right, left = (first, second) if group == "Z" else (second, first)
        lands_r, lands_l = {"X": (second, first), "Z": (second, first), "Y": (first, second)}[group]
        self.copies[group] = (
            r.push(self.out.at[k, right], self.inn.at[k, lands_r], self.send.at[2 * k], self.recv.at[2 * k], r.right),
            r.push(self.out.at[k, left], self.inn.at[k, lands_l], self.send.at[2 * k + 1], self.recv.at[2 * k + 1], r.left),
        )

    def arrived(self, group):
        for copy in self.copies[group]:
            copy.wait_recv()

    def finish(self):
        for pair in self.copies.values():
            for copy in pair:
                copy.wait_send()


def over_rows(rows, step, f):
    @pl.loop(0, rows // step)
    def _(i):
        f(pl.ds(pl.multiple_of(i * step, step), step))


def product(lhs, w, put, *, trans=False, tile):
    rows, k = lhs.shape
    cols = w.shape[0] if trans else w.shape[1]

    def body(ids, l_ref, w_ref):
        at = pl.multiple_of(ids.index[0] * tile, tile)
        put(pl.ds(at, tile), lax.dot_general(l_ref[...], w_ref[...], (((1,), (1 if trans else 0,)), ((), ())), preferred_element_type=F32))

    w_spec = pl.BlockSpec((tile, k), lambda j: (j, 0)) if trans else pl.BlockSpec((k, tile), lambda j: (0, j))
    pltpu.emit_pipeline(lambda ids, *refs: body(ids, *refs), grid=(cols // tile,), in_specs=[pl.BlockSpec((rows, k), lambda j: (0, 0)), w_spec],
                        _explicit_indices=True)(lhs, w)


def over_tokens(a, b, out, *, first=0, tile, wide=None):
    m, cols = out.shape
    wide = wide or cols
    sizes = [t.shape[0] for t in next(x for x in (a, b) if isinstance(x, list))]
    starts = [sum(sizes[:i]) for i in range(len(sizes))]
    pieces = lambda x: x if isinstance(x, list) else [x.at[pl.ds(s, z)] for s, z in zip(starts, sizes)]
    count = len(sizes)
    b = b if isinstance(b, list) else b.at[:, pl.ds(first, cols)]

    def body(*refs):
        parts = [lax.dot_general(l[...], r[...], (((0,), (0,)), ((), ())), preferred_element_type=F32) for l, r in zip(refs[:count], refs[count:])]
        refs[-1][...] = sum(parts[1:], parts[0]).astype(refs[-1].dtype)

    pltpu.emit_pipeline(body, grid=(cols // wide, m // tile),
                        in_specs=[pl.BlockSpec((z, tile), lambda j, i: (0, i)) for z in sizes] + [pl.BlockSpec((z, wide), lambda j, i: (0, j)) for z in sizes],
                        out_specs=[pl.BlockSpec((tile, wide), lambda j, i: (i, j))])(*pieces(a), *pieces(b), out)


def copy_all(*pairs):
    copies = [pltpu.make_async_copy(*p) for p in pairs]
    for c in copies:
        c.start()
    for c in copies:
        c.wait()


def call(kernel, name, number, count, outs, scratch, flops, size):
    return pl.pallas_call(
        kernel, name=name, in_specs=[ANY] * count, out_specs=[ANY] * len(outs), out_shape=outs, scratch_shapes=scratch,
        compiler_params=pltpu.CompilerParams(collective_id=number, has_side_effects=True, vmem_limit_bytes=60 * 2**20),
        cost_estimate=pl.CostEstimate(flops=flops, bytes_accessed=size, transcendentals=0),
    )


DMA6 = pltpu.SemaphoreType.DMA((6,))
DMA2 = pltpu.SemaphoreType.DMA((2,))


def shape(*dims, dtype=BF16):
    return jax.ShapeDtypeStruct(dims, dtype)


def gather_qkv(n, a, w):
    rows, d = a.shape
    cols = w.shape[1]

    def kernel(a, w, qkv, a_rest, part, send, recv, out_sem):
        ring = Ring(n, rows)
        ring.greet()
        g = Gather(ring, a, parts(a_rest, rows, "XYZ"), send, recv)
        g.step("X")
        g.step("Y")
        for group in "OXYZ":
            if group != "O":
                g.arrived(group)
            if group == "X":
                g.step("Z")

            def put(c, value):
                part[:, c] = value.astype(BF16)

            product(g.rows_of(group), w, put, tile=256)
            h = ring.half
            p0, p1 = ring.places(group)
            copy_all((part.at[pl.ds(0, h)], qkv.at[pl.ds(p0, h)], out_sem.at[0]), (part.at[pl.ds(h, h)], qkv.at[pl.ds(p1, h)], out_sem.at[1]))
        g.finish()

    run = call(kernel, "gather_qkv", 1, 2, (shape(n * rows, cols), shape((n - 1) * rows, d)),
                [pltpu.VMEM((rows, cols), BF16), DMA6, DMA6, DMA2], 2 * n * rows * d * cols, 2 * n * rows * d)
    return run(a, w)


def attention(n, qkv, cos, sin, kv_width, dy, *, bq=512, bk=384):
    tokens, width = qkv.shape[0], qkv.shape[1] - 2 * kv_width
    heads, (rows, d), low = width // HEAD, dy.shape, qkv.dtype
    bq, bk = _fit(tokens, bq), _fit(tokens, bk)

    def kernel(q_ref, k_ref, v_ref, cos_ref, sin_ref, dy, o_ref, lse_ref, dy_x, q_s, k_s, top_s, mix_s, gap_s, send, recv):
        ring = Ring(n, rows)
        h = ring.half
        top, bottom = pl.ds(0, h), pl.ds(h, h)
        copies = [ring.copy(dy.at[top], dy_x.at[top], send.at[0], recv.at[0], ring.right), ring.copy(dy.at[bottom], dy_x.at[bottom], send.at[1], recv.at[1], ring.left)]

        @pl.when(pl.program_id(0) == 0)
        def _():
            ring.greet()
            for c in copies:
                c.start()

        _forward(q_ref, k_ref, v_ref, cos_ref, sin_ref, o_ref, lse_ref, q_s, k_s, top_s, mix_s, gap_s, bk=bk)

        @pl.when(pl.program_id(0) == pl.num_programs(0) - 1)
        def _():
            for c in copies:
                c.wait()

    table = pl.BlockSpec((tokens, HEAD), lambda i: (0, 0))
    return pl.pallas_call(
        kernel, name="attention", grid=(tokens // bq,), in_specs=[*_views(qkv, width, kv_width, bq), table, table, ANY],
        out_specs=[pl.BlockSpec((bq, width), lambda i: (i, 0)), pl.BlockSpec((heads, bq), lambda i: (0, i)), ANY],
        out_shape=[shape(tokens, width), shape(heads, tokens, dtype=F32), shape(rows, d)],
        scratch_shapes=[pltpu.VMEM((bq, width), low), pltpu.VMEM((tokens, kv_width), low), pltpu.VMEM((heads, bq), F32), pltpu.VMEM((heads, HEAD + 8, bq), F32),
                        pltpu.VMEM((bk, bq), jnp.int32), DMA2, DMA2],
        compiler_params=pltpu.CompilerParams(dimension_semantics=("arbitrary",), collective_id=6, has_side_effects=True, vmem_limit_bytes=60 * 2**20),
        cost_estimate=pl.CostEstimate(flops=4 * heads * tokens * tokens * HEAD, transcendentals=heads * tokens * tokens, bytes_accessed=6 * tokens * width),
    )(qkv, qkv, qkv, cos, sin, dy)


def close(scatter, own, total):
    def f(r):
        total[r] = own[r] + scatter.inn[0, r].astype(F32) + scatter.inn[2, r].astype(F32)
    over_rows(scatter.ring.rows, 16, f)


def add_came(scatter, term):
    def f(r):
        scatter.out[2, r] = (term[r] + scatter.inn[1, r].astype(F32)).astype(BF16)
    over_rows(scatter.ring.rows, 16, f)


def scatter_out(n, heads, wo, dy, dy_x, w_down):
    tokens, width = heads.shape
    rows, d = dy.shape
    hidden = w_down.shape[0]

    def kernel(heads, wo, dy, dy_x, w_down, total_out, grouped, dy_rest, dh, wide, total, part, out_s, in_s, send, recv, s_send, s_recv, sem):
        ring = Ring(n, rows)
        h = ring.half
        ring.greet()
        sc = Scatter(ring, out_s, in_s, s_send, s_recv)
        g = Gather(ring, dy, parts(dy_rest, rows, "YZ"), send, recv, dy_x)
        index = {"O": 0, "X": 1, "Y": 2, "Z": 3}

        def term(group, target):
            p0, p1 = ring.places(group)
            at = index[group] * rows
            copy_all((heads.at[pl.ds(p0, h)], part.at[pl.ds(0, h)], sem.at[0]), (heads.at[pl.ds(p1, h)], part.at[pl.ds(h, h)], sem.at[1]))
            copy_all((part, grouped.at[pl.ds(at, rows)], sem.at[0]))
            product(grouped.at[pl.ds(at, rows)], wo, target, tile=512)

        def to_send(k):
            def put(c, value):
                out_s[k, :, c] = value.astype(BF16)
            return put

        def keep(c, value):
            total[:, c] = value

        def hid(group):
            def put(c, value):
                wide[:, c] = value.astype(BF16)
            product(g.rows_of(group), w_down, put, trans=True, tile=512)
            copy_all((wide, dh.at[pl.ds(index[group] * rows, rows)], sem.at[0]))

        term("X", to_send(0))
        sc.step("X")
        g.step("Y")
        term("Z", to_send(1))
        sc.step("Z")
        g.step("Z")
        term("Y", keep)
        hid("O")
        hid("X")
        sc.arrived("Z")
        add_came(sc, total)
        sc.step("Y")
        term("O", keep)
        g.arrived("Y")
        hid("Y")
        g.arrived("Z")
        hid("Z")
        sc.arrived("X")
        sc.arrived("Y")
        close(sc, total, total)
        copy_all((total, total_out, sem.at[0]))
        g.finish()
        sc.finish()

    run = call(kernel, "scatter_out", 2, 5, (shape(rows, d, dtype=F32), shape(tokens, width), shape((n - 2) * rows, d), shape(tokens, hidden)),
                [pltpu.VMEM((rows, hidden), BF16), pltpu.VMEM((rows, d), F32), pltpu.VMEM((rows, width), BF16), pltpu.VMEM((3, rows, d), BF16), pltpu.VMEM((3, rows, d), BF16),
                 DMA6, DMA6, DMA6, DMA6, DMA2], 2 * tokens * d * (width + hidden), 2 * tokens * d)
    return run(heads, wo, dy, dy_x, w_down)


def feed_forward(n, b, dh, w_gate, w_up):
    rows, d = b.shape
    tokens, width = dh.shape
    tile = 256

    def kernel(b, dh, w_gate, w_up, total_out, b_rest, hidden, d_gate, d_up, by_gate, total, own, held, out_s, in_s, send, recv, s_send, s_recv, sem):
        ring = Ring(n, rows)
        ring.greet()
        sc = Scatter(ring, out_s, in_s, s_send, s_recv)
        g = Gather(ring, b, parts(b_rest, rows, "XYZ"), send, recv)
        g.step("X")
        g.step("Y")

        def body(acc, ids, b_ref, dh_ref, wg_ref, wu_ref, hid_ref, dg_ref, du_ref):
            gate = lax.dot_general(b_ref[...], wg_ref[...], (((1,), (0,)), ((), ())), preferred_element_type=F32)
            up = lax.dot_general(b_ref[...], wu_ref[...], (((1,), (0,)), ((), ())), preferred_element_type=F32)
            s = 1 / (1 + jnp.exp(-gate))
            silu = gate * s
            by = dh_ref[...].astype(F32)
            hid_ref[...] = (silu * up).astype(BF16)
            dg = (by * up * (s + silu * (1 - s))).astype(BF16)
            du = (by * silu).astype(BF16)
            dg_ref[...] = dg
            du_ref[...] = du
            both = jnp.concatenate([dg, du], 1)

            @pl.when(ids.index[0] == 0)
            def _():
                acc[...] = jnp.zeros_like(acc)

            run = 512

            @pl.loop(0, d // run)
            def _(i):
                c = pl.ds(pl.multiple_of(i * run, run), run)
                w = jnp.concatenate([wg_ref[c, :], wu_ref[c, :]], 1)
                acc[:, c] += lax.dot_general(both, w, (((1,), (1,)), ((), ())), preferred_element_type=F32)

        def work(group, acc):
            at = pl.ds("OXYZ".index(group) * rows, rows)
            columns = pl.BlockSpec((rows, tile), lambda j: (0, j))
            weight = pl.BlockSpec((d, tile), lambda j: (0, j))
            pltpu.emit_pipeline(functools.partial(body, acc), grid=(width // tile,), in_specs=[pl.BlockSpec((rows, d), lambda j: (0, 0)), columns, weight, weight],
                                out_specs=[columns] * 3, _explicit_indices=True)(
                g.rows_of(group), dh.at[at], w_gate, w_up, hidden.at[at], d_gate.at[at], d_up.at[at])

        def to_send(k):
            def f(r):
                out_s[k, r] = total[r].astype(BF16)
            over_rows(rows, 16, f)

        work("O", own)
        g.arrived("X")
        g.step("Z")
        work("X", total)
        to_send(0)
        sc.step("X")
        g.arrived("Y")
        work("Y", held)
        g.arrived("Z")
        work("Z", total)
        to_send(1)
        sc.step("Z")
        over_tokens([b, b_rest], d_gate, by_gate, tile=512, wide=1024)
        sc.arrived("Z")
        add_came(sc, held)
        sc.step("Y")
        sc.arrived("X")
        sc.arrived("Y")
        close(sc, own, total)
        copy_all((total, total_out, sem.at[0]))
        g.finish()
        sc.finish()

    inner = shape(tokens, width)
    run = call(kernel, "feed_forward", 3, 4, (shape(rows, d, dtype=F32), shape(tokens - rows, d), inner, inner, inner, shape(d, width)),
                [pltpu.VMEM((rows, d), F32), pltpu.VMEM((rows, d), F32), pltpu.VMEM((rows, d), F32), pltpu.VMEM((3, rows, d), BF16), pltpu.VMEM((3, rows, d), BF16), DMA6, DMA6, DMA6, DMA6, DMA2],
                12 * tokens * d * width, 6 * d * width)
    return run(b, dh, w_gate, w_up)


def gather_heads(n, dh, wo, hidden, dy, dy_x, dy_rest, d_up, b, b_rest):
    rows, d = dh.shape
    width = wo.shape[0]
    inner = hidden.shape[1]

    def kernel(dh, wo, hidden, dy, dy_x, dy_rest, d_up, b, b_rest, d_heads, dh_rest, by_down, by_up, part, send, recv, sem):
        ring = Ring(n, rows)
        h = ring.half
        ring.greet()
        g = Gather(ring, dh, parts(dh_rest, rows, "XYZ"), send, recv)
        g.step("X")
        g.step("Y")

        def put(c, value):
            part[:, c] = value.astype(BF16)

        def work(group):
            product(g.rows_of(group), wo, put, trans=True, tile=256)
            p0, p1 = ring.places(group)
            copy_all((part.at[pl.ds(0, h)], d_heads.at[pl.ds(p0, h)], sem.at[0]), (part.at[pl.ds(h, h)], d_heads.at[pl.ds(p1, h)], sem.at[1]))

        work("O")
        over_tokens(hidden, [dy, dy_x, dy_rest], by_down, tile=512, wide=1024)
        g.arrived("X")
        g.step("Z")
        work("X")
        over_tokens([b, b_rest], d_up, by_up, tile=512, wide=1024)
        g.arrived("Y")
        work("Y")
        g.arrived("Z")
        work("Z")
        g.finish()

    run = call(kernel, "gather_heads", 4, 9,
                (shape(n * rows, width), shape((n - 1) * rows, d), shape(inner, d), shape(d, inner)),
                [pltpu.VMEM((rows, width), BF16), DMA6, DMA6, DMA2], 2 * n * rows * d * (width + inner), 2 * n * rows * d)
    return run(dh, wo, hidden, dy, dy_x, dy_rest, d_up, b, b_rest)


def scatter_in(n, dq, dk, dv, w, heads, dh, dh_rest, a, a_rest):
    (tokens, q_cols), k_cols, cols = dq.shape, dk.shape[1], w.shape[1]
    rows, d = dh.shape
    width = heads.shape[1]

    def kernel(dq, dk, dv, w, heads, dh, dh_rest, a, a_rest, total_out, grouped, by_q, by_k, by_v, by_o, total, part, out_s, in_s, s_send, s_recv, sem):
        ring = Ring(n, rows)
        h = ring.half
        ring.greet()
        sc = Scatter(ring, out_s, in_s, s_send, s_recv)
        columns = ((dq, pl.ds(0, q_cols)), (dk, pl.ds(q_cols, k_cols)), (dv, pl.ds(q_cols + k_cols, k_cols)))

        def term(group, target):
            p0, p1 = ring.places(group)
            at = pl.ds("OXYZ".index(group) * rows, rows)
            copy_all(*((t.at[pl.ds(p, h)], part.at[pl.ds(i * h, h), c], sem.at[2 * k + i]) for k, (t, c) in enumerate(columns) for i, p in enumerate((p0, p1))))
            copy_all((part, grouped.at[at], sem.at[0]))
            product(grouped.at[at], w, target, trans=True, tile=512)

        def to_send(k):
            def put(c, value):
                out_s[k, :, c] = value.astype(BF16)
            return put

        def keep(c, value):
            total[:, c] = value

        term("X", to_send(0))
        sc.step("X")
        term("Z", to_send(1))
        sc.step("Z")
        over_tokens(heads, [dh, dh_rest], by_o, tile=256, wide=1024)
        term("Y", keep)
        sc.arrived("Z")
        add_came(sc, total)
        sc.step("Y")
        term("O", keep)
        over_tokens([a, a_rest], grouped, by_q, tile=512)
        over_tokens([a, a_rest], grouped, by_k, first=q_cols, tile=512)
        over_tokens([a, a_rest], grouped, by_v, first=q_cols + k_cols, tile=512)
        sc.arrived("X")
        sc.arrived("Y")
        close(sc, total, total)
        copy_all((total, total_out, sem.at[0]))
        sc.finish()

    run = call(kernel, "scatter_in", 5, 9,
                (shape(rows, d, dtype=F32), shape(tokens, cols), shape(d, q_cols), shape(d, k_cols), shape(d, k_cols), shape(width, d)),
                [pltpu.VMEM((rows, d), F32), pltpu.VMEM((rows, cols), BF16), pltpu.VMEM((3, rows, d), BF16), pltpu.VMEM((3, rows, d), BF16), DMA6, DMA6, DMA6],
                4 * tokens * d * (cols + width), 2 * tokens * d)
    return run(dq, dk, dv, w, heads, dh, dh_rest, a, a_rest)


def solution(mesh):
    n = mesh.shape["tp"]

    def step(x, dy, wq, wk, wv, wo, w_gate, w_up, w_down):
        x, dy = x[0], dy[0]
        tokens = n * x.shape[0]
        wide_x = x.astype(F32)
        a = normed(wide_x)
        w = jnp.concatenate([wq, wk, wv], 1)
        qkv, a_rest = gather_qkv(n, a, w)
        cos, sin = tables(tokens)
        kv_width = wk.shape[1]
        out, lse, dy_x = attention(n, qkv, cos, sin, kv_width, dy)
        o, heads, dy_rest, d_hid = scatter_out(n, out, wo, dy, dy_x, w_down)
        wide_h = (wide_x + o).astype(BF16).astype(F32)
        b = normed(wide_h)
        db, b_rest, hidden, d_gate, d_up, by_gate = feed_forward(n, b, d_hid, w_gate, w_up)
        dh = (dy.astype(F32) + norm_back(wide_h, db)).astype(BF16)
        d_heads, dh_rest, by_down, by_up = gather_heads(n, dh, wo, hidden, dy, dy_x, dy_rest, d_up, b, b_rest)
        dq, dk, dv, by_gate, by_up, by_down = attention_back(qkv, cos, sin, d_heads, out, lse, kv_width, (by_gate, by_up, by_down))
        da, _, by_q, by_k, by_v, by_o = scatter_in(n, dq, dk, dv, w, heads, dh, dh_rest, a, a_rest)
        dx = (dh.astype(F32) + norm_back(wide_x, da)).astype(BF16)
        return dx[None], by_q, by_k, by_v, by_o, by_gate, by_up, by_down

    states, by_columns, by_rows = P("dp", "tp", None), P(None, "tp"), P("tp", None)
    weights = (by_columns, by_columns, by_columns, by_rows, by_columns, by_columns, by_rows)
    own = tuple(P("dp", "tp") if spec == by_columns else P(("dp", "tp"), None) for spec in weights)
    return jax.shard_map(step, mesh=mesh, in_specs=(states, states, *weights), out_specs=(states, *own), check_vma=False)
```

```python
import functools

import jax
import jax.numpy as jnp
from jax import lax
from jax.experimental import pallas as pl
from jax.experimental.pallas import tpu as pltpu

NEG = -1e30
HIDDEN = 2 * NEG
LOG2E = 1.4426950408889634
HEAD = 128


def _fit(size, want, unit=128):
    return max(n for n in range(unit, max(min(want, size), unit) + 1, unit) if size % n == 0)


def _dot(a, b, ca, cb):
    return lax.dot_general(a, b, (((ca,), (cb,)), ((), ())), preferred_element_type=jnp.float32)


def _turn(t, cos, sin, back=False):
    other = pltpu.roll(t, HEAD // 2, 1) * sin
    return t * cos - other if back else t * cos + other


def _blocks(iq, bq, bk, total):
    return lax.div(iq * bq + 1, bk), jnp.minimum(lax.div(iq * bq + bq - 1 + bk, bk), total)


def _gap(bk, bq):
    return lax.broadcasted_iota(jnp.int32, (bk, bq), 1) - lax.broadcasted_iota(jnp.int32, (bk, bq), 0)


def _cols(n):
    return slice(n * HEAD, (n + 1) * HEAD)


def _turn_keys(k_ref, cos_ref, sin_ref, k_s):
    step = 256

    @pl.loop(0, k_ref.shape[0] // step)
    def _(i):
        r = pl.ds(pl.multiple_of(i * step, step), step)
        for n in range(k_ref.shape[1] // HEAD):
            k_s[r, _cols(n)] = _turn(k_ref[r, _cols(n)].astype(jnp.float32), cos_ref[r, :], sin_ref[r, :]).astype(k_s.dtype)


def _turn_queries(iq, q_ref, cos_ref, sin_ref, q_s):
    bq = q_ref.shape[0]
    here = pl.ds(pl.multiple_of(iq * bq, bq), bq)
    for n in range(q_ref.shape[1] // HEAD):
        q_s[:, _cols(n)] = _turn(q_ref[:, _cols(n)].astype(jnp.float32), cos_ref[here, :], sin_ref[here, :]).astype(q_s.dtype)


def _forward(q_ref, k_ref, v_ref, cos_ref, sin_ref, o_ref, lse_ref, q_s, k_s, top_s, mix_s, gap_s, *, bk):
    bq, heads, kv = q_ref.shape[0], q_ref.shape[1] // HEAD, k_ref.shape[1] // HEAD
    g, scale = heads // kv, HEAD**-0.5
    e, low = scale * LOG2E, q_ref.dtype
    iq = pl.program_id(0)

    @pl.when(iq == 0)
    def _():
        gap_s[...] = _gap(bk, bq)
        _turn_keys(k_ref, cos_ref, sin_ref, k_s)

    _turn_queries(iq, q_ref, cos_ref, sin_ref, q_s)
    top_s[...] = jnp.full_like(top_s, NEG)
    mix_s[...] = jnp.zeros_like(mix_s)
    ones = jnp.ones((8, bk), low)

    def block(j, masked):
        here = pl.ds(pl.multiple_of(j * bk, bk), bk)
        scores = [_dot(k_s[here, _cols(n // g)], q_s[:, _cols(n)], 1, 1) for n in range(heads)]
        ok = gap_s[...] >= j * bk - iq * bq if masked else None
        weights, keeps = [], []
        for n, s in enumerate(scores):
            if masked:
                s = jnp.where(ok, s, HIDDEN)
            old = top_s[n : n + 1, :]
            top = jnp.maximum(old, s.max(axis=0, keepdims=True))
            top_s[n : n + 1, :] = top
            weights.append(jnp.exp2((s - top) * e).astype(low))
            keeps.append(jnp.exp2((old - top) * e))
        for n, (p, keep) in enumerate(zip(weights, keeps)):
            values = jnp.concatenate([v_ref[here, _cols(n // g)].T, ones], axis=0)
            mix_s[n] = mix_s[n] * keep + _dot(values, p, 1, 0)

    whole, last = _blocks(iq, bq, bk, k_ref.shape[0] // bk)
    lax.fori_loop(0, whole, lambda j, _: block(j, False), None)
    lax.fori_loop(whole, last, lambda j, _: block(j, True), None)
    for n in range(heads):
        total = mix_s[n, HEAD : HEAD + 1, :]
        o_ref[:, _cols(n)] = (mix_s[n, :HEAD, :] * (1 / total)).T.astype(o_ref.dtype)
        lse_ref[n : n + 1, :] = top_s[n : n + 1, :] * scale + jnp.log(total)


def _backward(q_ref, k_ref, v_ref, cos_ref, sin_ref, do_ref, o_ref, lse_ref, *rest, bk, moved):
    given, rest = rest[:moved], rest[moved:]
    dq_ref, dk_ref, dv_ref = rest[:3]
    taken, (q_s, k_s, dq_s, dk_s, dv_s, gap_s, sem) = rest[3 : 3 + moved], rest[3 + moved :]
    bq, heads, kv = q_ref.shape[0], q_ref.shape[1] // HEAD, k_ref.shape[1] // HEAD
    g, scale = heads // kv, HEAD**-0.5
    e, low = scale * LOG2E, q_ref.dtype
    iq = pl.program_id(0)

    @pl.when(iq == 0)
    def _():
        gap_s[...] = _gap(bk, bq)
        _turn_keys(k_ref, cos_ref, sin_ref, k_s)
        dk_s[...] = jnp.zeros_like(dk_s)
        dv_s[...] = jnp.zeros_like(dv_s)

    _turn_queries(iq, q_ref, cos_ref, sin_ref, q_s)
    dq_s[...] = jnp.zeros_like(dq_s)
    copies = []
    for i, (source, target) in enumerate(zip(given, taken)):
        r, c = source.shape
        here = pl.ds(pl.multiple_of(iq * r, r), r), slice(None)
        if r == target.shape[0]:
            here = slice(None), pl.ds(pl.multiple_of(iq * c, c), c)
        copies.append(pltpu.make_async_copy(source, target.at[here], sem.at[i]))
        copies[-1].start()
    lses, deltas = [], []
    for n in range(heads):
        both = do_ref[:, _cols(n)].astype(jnp.float32) * o_ref[:, _cols(n)].astype(jnp.float32)
        deltas.append(both.T.sum(axis=0, keepdims=True))
        lses.append(lse_ref[n : n + 1, :] * LOG2E)

    def block(j, masked):
        here = pl.ds(pl.multiple_of(j * bk, bk), bk)
        scores = [_dot(k_s[here, _cols(n // g)], q_s[:, _cols(n)], 1, 1) for n in range(heads)]
        dps = [_dot(v_ref[here, _cols(n // g)], do_ref[:, _cols(n)], 1, 1) for n in range(heads)]
        ok = gap_s[...] >= j * bk - iq * bq if masked else None
        for n in range(heads):
            p = jnp.exp2(scores[n] * e - lses[n])
            if masked:
                p = jnp.where(ok, p, 0.0)
            ds = (p * (dps[n] - deltas[n])).astype(low)
            c = _cols(n // g)
            dv_s[here, c] += _dot(p.astype(low), do_ref[:, _cols(n)], 1, 0)
            dk_s[here, c] += _dot(ds, q_s[:, _cols(n)], 1, 0)
            dq_s[n] += _dot(k_s[here, c].T, ds, 1, 0)

    whole, last = _blocks(iq, bq, bk, k_ref.shape[0] // bk)
    lax.fori_loop(0, whole, lambda j, _: block(j, False), None)
    lax.fori_loop(whole, last, lambda j, _: block(j, True), None)
    mine = pl.ds(pl.multiple_of(iq * bq, bq), bq)
    for n in range(heads):
        dq_ref[:, _cols(n)] = _turn((dq_s[n] * scale).T, cos_ref[mine, :], sin_ref[mine, :], True).astype(dq_ref.dtype)

    for copy in copies:
        copy.wait()

    @pl.when(iq == pl.num_programs(0) - 1)
    def _():
        step = 256

        @pl.loop(0, dk_s.shape[0] // step)
        def _(i):
            r = pl.ds(pl.multiple_of(i * step, step), step)
            dv_ref[r, :] = dv_s[r, :].astype(dv_ref.dtype)
            for n in range(kv):
                dk_ref[r, _cols(n)] = _turn(dk_s[r, _cols(n)] * scale, cos_ref[r, :], sin_ref[r, :], True).astype(dk_ref.dtype)


def _views(qkv, width, kv_width, bq):
    tokens = qkv.shape[0]
    at = width // kv_width
    return [pl.BlockSpec((bq, width), lambda i: (i, 0)), pl.BlockSpec((tokens, kv_width), lambda i: (0, at)), pl.BlockSpec((tokens, kv_width), lambda i: (0, at + 1))]


def attention_back(qkv, cos, sin, d_out, out, lse, kv_width, pass_on, *, bq=256, bk=256):
    tokens, width = d_out.shape
    heads = width // HEAD
    bq, bk = _fit(tokens, bq), _fit(tokens, bk)
    steps = tokens // bq
    mine = pl.BlockSpec((bq, width), lambda i: (i, 0))
    table = pl.BlockSpec((tokens, HEAD), lambda i: (0, 0))
    keys = pl.BlockSpec((tokens, kv_width), lambda i: (0, 0))
    runs = [pl.BlockSpec((t.shape[0] // steps, t.shape[1]), lambda i: (i, 0)) if t.shape[0] % (16 * steps) == 0 else pl.BlockSpec((t.shape[0], t.shape[1] // steps), lambda i: (0, i))
            for t in pass_on]
    low = qkv.dtype
    return pl.pallas_call(
        functools.partial(_backward, bk=bk, moved=len(pass_on)), name="attention_back", grid=(steps,),
        in_specs=[*_views(qkv, width, kv_width, bq), table, table, mine, mine, pl.BlockSpec((heads, bq), lambda i: (0, i)), *runs],
        out_specs=[mine, keys, keys, *(pl.BlockSpec(memory_space=pl.ANY) for _ in pass_on)],
        out_shape=[jax.ShapeDtypeStruct((tokens, width), low), jax.ShapeDtypeStruct((tokens, kv_width), low), jax.ShapeDtypeStruct((tokens, kv_width), low),
                   *(jax.ShapeDtypeStruct(t.shape, t.dtype) for t in pass_on)],
        scratch_shapes=[pltpu.VMEM((bq, width), low), pltpu.VMEM((tokens, kv_width), low), pltpu.VMEM((heads, HEAD, bq), jnp.float32),
                        pltpu.VMEM((tokens, kv_width), jnp.float32), pltpu.VMEM((tokens, kv_width), jnp.float32), pltpu.VMEM((bk, bq), jnp.int32),
                        pltpu.SemaphoreType.DMA((max(len(pass_on), 1),))],
        compiler_params=pltpu.CompilerParams(dimension_semantics=("arbitrary",), vmem_limit_bytes=60 * 2**20),
        cost_estimate=pl.CostEstimate(flops=10 * heads * tokens * tokens * HEAD, transcendentals=heads * tokens * tokens, bytes_accessed=8 * tokens * width),
    )(qkv, qkv, qkv, cos, sin, d_out, out, lse, *pass_on)

from jax.sharding import PartitionSpec as P

THETA = 10000
BF16, F32 = jnp.bfloat16, jnp.float32
MESH = pl.DeviceIdType.MESH
ANY = pl.BlockSpec(memory_space=pl.ANY)


def norm_scale(wide):
    return lax.rsqrt(jnp.mean(wide**2, -1, keepdims=True) + 1e-6)


def normed(wide):
    return (wide * norm_scale(wide)).astype(BF16)


def norm_back(wide, by_out):
    scale = norm_scale(wide)
    along = jnp.mean(wide * by_out, -1, keepdims=True)
    return scale * by_out - wide * (along * scale**3)


def tables(tokens):
    half = HEAD // 2
    angle = jnp.arange(tokens, dtype=F32)[:, None] * THETA ** (-(jnp.arange(HEAD) % half).astype(F32) / half)
    return jnp.cos(angle), jnp.sin(angle) * jnp.where(jnp.arange(HEAD) < half, -1.0, 1.0)


class Ring:
    def __init__(self, n, rows):
        self.n, self.rows, self.half = n, rows, rows // 2
        self.me = lax.axis_index("tp")
        self.right, self.left = lax.rem(self.me + 1, n), lax.rem(self.me + n - 1, n)
        self.across = lax.rem(self.me + 2, n)

    def greet(self):
        barrier = pltpu.get_barrier_semaphore()
        for to in (self.left, self.right):
            pl.semaphore_signal(barrier, inc=1, device_id={"tp": to}, device_id_type=MESH)
        pl.semaphore_wait(barrier, 2)

    def copy(self, src, dst, send, recv, to):
        return pltpu.make_async_remote_copy(src_ref=src, dst_ref=dst, send_sem=send, recv_sem=recv, device_id={"tp": to}, device_id_type=MESH)

    def push(self, *where):
        copy = self.copy(*where)
        copy.start()
        return copy

    def places(self, group):
        rows, half = self.rows, self.half
        return {
            "O": (self.me * rows, self.me * rows + half),
            "X": (self.left * rows, self.right * rows + half),
            "Y": (self.left * rows + half, self.right * rows),
            "Z": (self.across * rows, self.across * rows + half),
        }[group]


class Gather:
    def __init__(self, ring, own, at, send, recv, first=None):
        self.ring, self.own, self.send, self.recv, self.copies = ring, own, send, recv, {}
        self.at = dict(at, O=own) if first is None else dict(at, O=own, X=first)

    def step(self, group):
        r, h = self.ring, self.ring.half
        top, bottom = pl.ds(0, h), pl.ds(h, h)
        k = 2 * "XYZ".index(group)
        source = self.at["X" if group == "Z" else "O"]
        right, left = (bottom, top) if group == "Y" else (top, bottom)
        self.copies[group] = (
            r.push(source.at[right], self.at[group].at[top], self.send.at[k], self.recv.at[k], r.right),
            r.push(source.at[left], self.at[group].at[bottom], self.send.at[k + 1], self.recv.at[k + 1], r.left),
        )

    def arrived(self, group):
        for copy in self.copies[group]:
            copy.wait_recv()

    def finish(self):
        for pair in self.copies.values():
            for copy in pair:
                copy.wait_send()

    def rows_of(self, group):
        return self.at[group]


def parts(ref, rows, groups):
    return {group: ref.at[pl.ds(i * rows, rows)] for i, group in enumerate(groups)}


class Scatter:
    def __init__(self, ring, out_s, in_s, send, recv):
        self.ring, self.out, self.inn, self.send, self.recv, self.copies = ring, out_s, in_s, send, recv, {}

    def step(self, group):
        r, h = self.ring, self.ring.half
        k = "XZY".index(group)
        first, second = pl.ds(0, h), pl.ds(h, h)
        right, left = (first, second) if group == "Z" else (second, first)
        lands_r, lands_l = {"X": (second, first), "Z": (second, first), "Y": (first, second)}[group]
        self.copies[group] = (
            r.push(self.out.at[k, right], self.inn.at[k, lands_r], self.send.at[2 * k], self.recv.at[2 * k], r.right),
            r.push(self.out.at[k, left], self.inn.at[k, lands_l], self.send.at[2 * k + 1], self.recv.at[2 * k + 1], r.left),
        )

    def arrived(self, group):
        for copy in self.copies[group]:
            copy.wait_recv()

    def finish(self):
        for pair in self.copies.values():
            for copy in pair:
                copy.wait_send()


def over_rows(rows, step, f):
    @pl.loop(0, rows // step)
    def _(i):
        f(pl.ds(pl.multiple_of(i * step, step), step))


def product(lhs, w, put, *, trans=False, tile):
    @pl.loop(0, w.shape[0 if trans else 1] // tile)
    def _(i):
        c = pl.ds(pl.multiple_of(i * tile, tile), tile)
        put(c, _dot(lhs[...], w[c, :], 1, 1) if trans else _dot(lhs[...], w[:, c], 1, 0))


def over_tokens(a, b, outs, *, tile, wide=None):
    widths = [o.shape[1] for o in outs]
    wide = wide or sum(widths)
    ends = [sum(widths[: i + 1]) for i in range(len(widths))]

    def body(l, r, *targets):
        whole = _dot(l[...], r[...], 0, 0).astype(BF16)
        for target, end in zip(targets, ends):
            target[...] = whole if len(outs) == 1 else whole[:, end - target.shape[1] : end]

    tokens, m = a.shape
    pltpu.emit_pipeline(body, grid=(b.shape[1] // wide, m // tile),
                        in_specs=[pl.BlockSpec((tokens, tile), lambda j, i: (0, i)), pl.BlockSpec((tokens, wide), lambda j, i: (0, j))],
                        out_specs=[pl.BlockSpec((tile, wide if len(outs) == 1 else w), lambda j, i: (i, j)) for w in widths])(a, b, *outs)


def copy_all(*pairs):
    copies = [pltpu.make_async_copy(*p) for p in pairs]
    for c in copies:
        c.start()
    for c in copies:
        c.wait()


def call(kernel, name, number, count, outs, scratch, flops, size):
    return pl.pallas_call(
        kernel, name=name, in_specs=[ANY] * count, out_specs=[ANY] * len(outs), out_shape=outs, scratch_shapes=scratch,
        compiler_params=pltpu.CompilerParams(collective_id=number, has_side_effects=True, vmem_limit_bytes=60 * 2**20),
        cost_estimate=pl.CostEstimate(flops=flops, bytes_accessed=size, transcendentals=0),
    )


DMA6 = pltpu.SemaphoreType.DMA((6,))
DMA2 = pltpu.SemaphoreType.DMA((2,))


def shape(*dims, dtype=BF16):
    return jax.ShapeDtypeStruct(dims, dtype)


def gather_qkv(n, a, wq, wk, wv):
    rows, d = a.shape
    widths = [t.shape[1] for t in (wq, wk, wv)]
    cols = sum(widths)

    def kernel(a, wq, wk, wv, qkv, a_all, w, lhs, part, send, recv, sem):
        ring = Ring(n, rows)
        h = ring.half
        ring.greet()
        all_parts = parts(a_all, rows, "OXYZ")
        g = Gather(ring, a, all_parts, send, recv)
        g.step("X")
        g.step("Y")
        copy_all((a, lhs, sem.at[0]), *((t, w.at[:, pl.ds(sum(widths[:i]), widths[i])], sem.at[i + 1]) for i, t in enumerate((wq, wk, wv))))
        copy_all((lhs, all_parts["O"], sem.at[0]))
        for group in "OXYZ":
            if group != "O":
                g.arrived(group)
                if group == "X":
                    g.step("Z")
                copy_all((g.rows_of(group), lhs, sem.at[0]))

            def put(c, value):
                part[:, c] = value.astype(BF16)

            product(lhs, w, put, tile=256)
            p0, p1 = ring.places(group)
            copy_all((part.at[pl.ds(0, h)], qkv.at[pl.ds(p0, h)], sem.at[0]), (part.at[pl.ds(h, h)], qkv.at[pl.ds(p1, h)], sem.at[1]))
        g.finish()

    run = call(kernel, "gather_qkv", 1, 4, (shape(n * rows, cols), shape(n * rows, d)),
               [pltpu.VMEM((d, cols), BF16), pltpu.VMEM((rows, d), BF16), pltpu.VMEM((rows, cols), BF16), DMA6, DMA6, DMA6], 2 * n * rows * d * cols, 2 * n * rows * d)
    return run(a, wq, wk, wv)


def attention(n, qkv, cos, sin, kv_width, dy, *, bq=512, bk=384):
    tokens, width = qkv.shape[0], qkv.shape[1] - 2 * kv_width
    heads, (rows, d), low = width // HEAD, dy.shape, qkv.dtype
    bq, bk = _fit(tokens, bq), _fit(tokens, bk)

    def kernel(q_ref, k_ref, v_ref, cos_ref, sin_ref, dy, o_ref, lse_ref, dy_x, q_s, k_s, top_s, mix_s, gap_s, send, recv):
        ring = Ring(n, rows)
        h = ring.half
        top, bottom = pl.ds(0, h), pl.ds(h, h)
        copies = [ring.copy(dy.at[top], dy_x.at[top], send.at[0], recv.at[0], ring.right), ring.copy(dy.at[bottom], dy_x.at[bottom], send.at[1], recv.at[1], ring.left)]

        @pl.when(pl.program_id(0) == 0)
        def _():
            ring.greet()
            for c in copies:
                c.start()

        _forward(q_ref, k_ref, v_ref, cos_ref, sin_ref, o_ref, lse_ref, q_s, k_s, top_s, mix_s, gap_s, bk=bk)

        @pl.when(pl.program_id(0) == pl.num_programs(0) - 1)
        def _():
            for c in copies:
                c.wait()

    table = pl.BlockSpec((tokens, HEAD), lambda i: (0, 0))
    return pl.pallas_call(
        kernel, name="attention", grid=(tokens // bq,), in_specs=[*_views(qkv, width, kv_width, bq), table, table, ANY],
        out_specs=[pl.BlockSpec((bq, width), lambda i: (i, 0)), pl.BlockSpec((heads, bq), lambda i: (0, i)), ANY],
        out_shape=[shape(tokens, width), shape(heads, tokens, dtype=F32), shape(rows, d)],
        scratch_shapes=[pltpu.VMEM((bq, width), low), pltpu.VMEM((tokens, kv_width), low), pltpu.VMEM((heads, bq), F32), pltpu.VMEM((heads, HEAD + 8, bq), F32),
                        pltpu.VMEM((bk, bq), jnp.int32), DMA2, DMA2],
        compiler_params=pltpu.CompilerParams(dimension_semantics=("arbitrary",), collective_id=6, has_side_effects=True, vmem_limit_bytes=60 * 2**20),
        cost_estimate=pl.CostEstimate(flops=4 * heads * tokens * tokens * HEAD, transcendentals=heads * tokens * tokens, bytes_accessed=6 * tokens * width),
    )(qkv, qkv, qkv, cos, sin, dy)


def close(scatter, own, total):
    def f(r):
        total[r] = own[r] + scatter.inn[0, r].astype(F32) + scatter.inn[2, r].astype(F32)
    over_rows(scatter.ring.rows, 16, f)


def add_came(scatter, term):
    def f(r):
        scatter.out[2, r] = (term[r] + scatter.inn[1, r].astype(F32)).astype(BF16)
    over_rows(scatter.ring.rows, 16, f)


def scatter_out(n, heads, wo, dy, dy_x, w_down):
    tokens, width = heads.shape
    rows, d = dy.shape
    hidden = w_down.shape[0]

    def kernel(heads, wo, dy, dy_x, w_down, total_out, grouped, dy_all, dh, w, lhs, wide, total, part, out_s, in_s, send, recv, s_send, s_recv, sem):
        ring = Ring(n, rows)
        h = ring.half
        ring.greet()
        sc = Scatter(ring, out_s, in_s, s_send, s_recv)
        all_parts = parts(dy_all, rows, "OXYZ")
        g = Gather(ring, dy, all_parts, send, recv, dy_x)
        copy_all((wo, w, sem.at[0]))

        def term(group, target):
            p0, p1 = ring.places(group)
            at = pl.ds("OXYZ".index(group) * rows, rows)
            copy_all((heads.at[pl.ds(p0, h)], part.at[pl.ds(0, h)], sem.at[0]), (heads.at[pl.ds(p1, h)], part.at[pl.ds(h, h)], sem.at[1]))
            copy_all((part, grouped.at[at], sem.at[0]))
            product(part, w, target, tile=512)

        def to_send(k):
            def put(c, value):
                out_s[k, :, c] = value.astype(BF16)
            return put

        def keep(c, value):
            total[:, c] = value

        def hid(group):
            copy_all((g.rows_of(group), lhs, sem.at[0]))
            if group in "OX":
                copy_all((lhs, all_parts[group], sem.at[0]))

            def body(step, w_ref):
                c = pl.ds(pl.multiple_of(step.index[0] * 512, 512), 512)
                wide[:, c] = _dot(lhs[...], w_ref[...], 1, 1).astype(BF16)

            pltpu.emit_pipeline(body, grid=(hidden // 512,), in_specs=[pl.BlockSpec((512, d), lambda j: (j, 0))], _explicit_indices=True)(w_down)
            copy_all((wide, dh.at[pl.ds("OXYZ".index(group) * rows, rows)], sem.at[0]))

        term("X", to_send(0))
        sc.step("X")
        g.step("Y")
        term("Z", to_send(1))
        sc.step("Z")
        g.step("Z")
        term("Y", keep)
        hid("O")
        hid("X")
        sc.arrived("Z")
        add_came(sc, total)
        sc.step("Y")
        term("O", keep)
        g.arrived("Y")
        hid("Y")
        g.arrived("Z")
        hid("Z")
        sc.arrived("X")
        sc.arrived("Y")
        close(sc, total, total)
        copy_all((total, total_out, sem.at[0]))
        g.finish()
        sc.finish()

    run = call(kernel, "scatter_out", 2, 5, (shape(rows, d, dtype=F32), shape(tokens, width), shape(tokens, d), shape(tokens, hidden)),
                [pltpu.VMEM((width, d), BF16), pltpu.VMEM((rows, d), BF16), pltpu.VMEM((rows, hidden), BF16), pltpu.VMEM((rows, d), F32), pltpu.VMEM((rows, width), BF16), pltpu.VMEM((3, rows, d), BF16), pltpu.VMEM((3, rows, d), BF16),
                 DMA6, DMA6, DMA6, DMA6, DMA2], 2 * tokens * d * (width + hidden), 2 * tokens * d)
    return run(heads, wo, dy, dy_x, w_down)


def feed_forward(n, b, dh, w_gate, w_up):
    rows, d = b.shape
    tokens, width = dh.shape
    tile = 512

    def kernel(b, dh, w_gate, w_up, total_out, b_all, hidden, d_gate, d_up, by_gate, total, own, out_s, in_s, send, recv, s_send, s_recv, sem):
        ring = Ring(n, rows)
        ring.greet()
        sc = Scatter(ring, out_s, in_s, s_send, s_recv)
        g = Gather(ring, b, parts(b_all, rows, "OXYZ"), send, recv)
        g.step("X")
        g.step("Y")
        copy_all((b, out_s.at[0], sem.at[0]))
        copy_all((out_s.at[0], b_all.at[pl.ds(0, rows)], sem.at[0]))

        def body(acc, ids, b_ref, dh_ref, wg_ref, wu_ref, hid_ref, dg_ref, du_ref):
            gate = lax.dot_general(b_ref[...], wg_ref[...], (((1,), (0,)), ((), ())), preferred_element_type=F32)
            up = lax.dot_general(b_ref[...], wu_ref[...], (((1,), (0,)), ((), ())), preferred_element_type=F32)
            s = 1 / (1 + jnp.exp(-gate))
            silu = gate * s
            by = dh_ref[...].astype(F32)
            hid_ref[...] = (silu * up).astype(BF16)
            dg = (by * up * (s + silu * (1 - s))).astype(BF16)
            du = (by * silu).astype(BF16)
            dg_ref[...] = dg
            du_ref[...] = du

            @pl.when(ids.index[0] == 0)
            def _():
                acc[...] = jnp.zeros_like(acc)

            acc[...] += _dot(dg, wg_ref[...], 1, 1) + _dot(du, wu_ref[...], 1, 1)

        def work(group, acc):
            at = pl.ds("OXYZ".index(group) * rows, rows)
            columns = pl.BlockSpec((rows, tile), lambda j: (0, j))
            weight = pl.BlockSpec((d, tile), lambda j: (0, j))
            pltpu.emit_pipeline(functools.partial(body, acc), grid=(width // tile,), in_specs=[pl.BlockSpec((rows, d), lambda j: (0, 0)), columns, weight, weight],
                                out_specs=[columns] * 3, _explicit_indices=True)(
                g.rows_of(group), dh.at[at], w_gate, w_up, hidden.at[at], d_gate.at[at], d_up.at[at])

        def to_send(k):
            def f(r):
                out_s[k, r] = total[r].astype(BF16)
            over_rows(rows, 16, f)

        work("O", own)
        g.arrived("X")
        g.step("Z")
        work("X", total)
        to_send(0)
        sc.step("X")
        g.arrived("Z")
        work("Z", total)
        to_send(1)
        sc.step("Z")
        g.arrived("Y")
        work("Y", total)
        sc.arrived("Z")
        add_came(sc, total)
        sc.step("Y")
        over_tokens(b_all, d_gate, [by_gate], tile=1024, wide=1024)
        sc.arrived("X")
        sc.arrived("Y")
        close(sc, own, total)
        copy_all((total, total_out, sem.at[0]))
        g.finish()
        sc.finish()

    inner = shape(tokens, width)
    run = call(kernel, "feed_forward", 3, 4, (shape(rows, d, dtype=F32), shape(tokens, d), inner, inner, inner, shape(d, width)),
                [pltpu.VMEM((rows, d), F32), pltpu.VMEM((rows, d), F32), pltpu.VMEM((3, rows, d), BF16), pltpu.VMEM((3, rows, d), BF16), DMA6, DMA6, DMA6, DMA6, DMA2],
                12 * tokens * d * width, 6 * d * width)
    return run(b, dh, w_gate, w_up)


def gather_heads(n, dh, wo, hidden, dy_all, d_up, b_all):
    rows, d = dh.shape
    width = wo.shape[0]
    inner = hidden.shape[1]

    def kernel(dh, wo, hidden, dy_all, d_up, b_all, d_heads, dh_all, by_down, by_up, w, lhs, part, send, recv, sem):
        ring = Ring(n, rows)
        h = ring.half
        ring.greet()
        all_parts = parts(dh_all, rows, "OXYZ")
        g = Gather(ring, dh, all_parts, send, recv)
        g.step("X")
        g.step("Y")
        copy_all((wo, w, sem.at[0]))

        def put(c, value):
            part[:, c] = value.astype(BF16)

        def work(group):
            copy_all((g.rows_of(group), lhs, sem.at[0]))
            if group == "O":
                copy_all((lhs, all_parts["O"], sem.at[0]))
            product(lhs, w, put, trans=True, tile=256)
            p0, p1 = ring.places(group)
            copy_all((part.at[pl.ds(0, h)], d_heads.at[pl.ds(p0, h)], sem.at[0]), (part.at[pl.ds(h, h)], d_heads.at[pl.ds(p1, h)], sem.at[1]))

        work("O")
        over_tokens(hidden, dy_all, [by_down], tile=1024, wide=1024)
        g.arrived("X")
        g.step("Z")
        work("X")
        over_tokens(b_all, d_up, [by_up], tile=1024, wide=1024)
        g.arrived("Y")
        work("Y")
        g.arrived("Z")
        work("Z")
        g.finish()

    run = call(kernel, "gather_heads", 4, 6,
                (shape(n * rows, width), shape(n * rows, d), shape(inner, d), shape(d, inner)),
                [pltpu.VMEM((width, d), BF16), pltpu.VMEM((rows, d), BF16), pltpu.VMEM((rows, width), BF16), DMA6, DMA6, DMA2], 2 * n * rows * d * (width + inner), 2 * n * rows * d)
    return run(dh, wo, hidden, dy_all, d_up, b_all)


def scatter_in(n, dq, dk, dv, wq, wk, wv, heads, dh_all, a_all):
    (tokens, q_cols), k_cols, d = dq.shape, dk.shape[1], wq.shape[0]
    rows, cols = tokens // n, q_cols + 2 * k_cols
    width = heads.shape[1]

    def kernel(dq, dk, dv, wq, wk, wv, heads, dh_all, a_all, total_out, grouped, by_q, by_k, by_v, by_o, w, total, part, out_s, in_s, s_send, s_recv, sem):
        ring = Ring(n, rows)
        h = ring.half
        ring.greet()
        sc = Scatter(ring, out_s, in_s, s_send, s_recv)
        columns = ((dq, pl.ds(0, q_cols)), (dk, pl.ds(q_cols, k_cols)), (dv, pl.ds(q_cols + k_cols, k_cols)))
        copy_all(*((t, w.at[:, c], sem.at[k]) for k, (t, (_, c)) in enumerate(zip((wq, wk, wv), columns))))

        def term(group, target):
            p0, p1 = ring.places(group)
            at = pl.ds("OXYZ".index(group) * rows, rows)
            copy_all(*((t.at[pl.ds(p, h)], part.at[pl.ds(i * h, h), c], sem.at[2 * k + i]) for k, (t, c) in enumerate(columns) for i, p in enumerate((p0, p1))))
            copy_all((part, grouped.at[at], sem.at[0]))
            product(part, w, target, trans=True, tile=512)

        def to_send(k):
            def put(c, value):
                out_s[k, :, c] = value.astype(BF16)
            return put

        def keep(c, value):
            total[:, c] = value

        term("X", to_send(0))
        sc.step("X")
        term("Z", to_send(1))
        sc.step("Z")
        term("Y", keep)
        over_tokens(heads, dh_all, [by_o], tile=width, wide=1024)
        sc.arrived("Z")
        add_came(sc, total)
        sc.step("Y")
        term("O", keep)
        over_tokens(a_all, grouped, [by_q, by_k, by_v], tile=512)
        sc.arrived("X")
        sc.arrived("Y")
        close(sc, total, total)
        copy_all((total, total_out, sem.at[0]))
        sc.finish()

    run = call(kernel, "scatter_in", 5, 9,
                (shape(rows, d, dtype=F32), shape(tokens, cols), shape(d, q_cols), shape(d, k_cols), shape(d, k_cols), shape(width, d)),
                [pltpu.VMEM((d, cols), BF16), pltpu.VMEM((rows, d), F32), pltpu.VMEM((rows, cols), BF16), pltpu.VMEM((3, rows, d), BF16), pltpu.VMEM((3, rows, d), BF16), DMA6, DMA6, DMA6],
                4 * tokens * d * (cols + width), 2 * tokens * d)
    return run(dq, dk, dv, wq, wk, wv, heads, dh_all, a_all)


def solution(mesh):
    n = mesh.shape["tp"]

    def step(x, dy, wq, wk, wv, wo, w_gate, w_up, w_down):
        x, dy = x[0], dy[0]
        tokens = n * x.shape[0]
        wide_x = x.astype(F32)
        a = normed(wide_x)
        qkv, a_all = gather_qkv(n, a, wq, wk, wv)
        cos, sin = tables(tokens)
        kv_width = wk.shape[1]
        out, lse, dy_x = attention(n, qkv, cos, sin, kv_width, dy)
        o, heads, dy_all, d_hid = scatter_out(n, out, wo, dy, dy_x, w_down)
        wide_h = (wide_x + o).astype(BF16).astype(F32)
        b = normed(wide_h)
        db, b_all, hidden, d_gate, d_up, by_gate = feed_forward(n, b, d_hid, w_gate, w_up)
        dh = (dy.astype(F32) + norm_back(wide_h, db)).astype(BF16)
        d_heads, dh_all, by_down, by_up = gather_heads(n, dh, wo, hidden, dy_all, d_up, b_all)
        dq, dk, dv, by_gate, by_up, by_down = attention_back(qkv, cos, sin, d_heads, out, lse, kv_width, (by_gate, by_up, by_down))
        da, _, by_q, by_k, by_v, by_o = scatter_in(n, dq, dk, dv, wq, wk, wv, heads, dh_all, a_all)
        dx = (dh.astype(F32) + norm_back(wide_x, da)).astype(BF16)
        return dx[None], by_q, by_k, by_v, by_o, by_gate, by_up, by_down

    states, by_columns, by_rows = P("dp", "tp", None), P(None, "tp"), P("tp", None)
    weights = (by_columns, by_columns, by_columns, by_rows, by_columns, by_columns, by_rows)
    own = tuple(P("dp", "tp") if spec == by_columns else P(("dp", "tp"), None) for spec in weights)
    return jax.shard_map(step, mesh=mesh, in_specs=(states, states, *weights), out_specs=(states, *own), check_vma=False)
```

```python
import functools

import jax
import jax.numpy as jnp
import numpy as np
from jax import lax
from jax.experimental import pallas as pl
from jax.experimental.pallas import tpu as pltpu

NEG = -1e30
HIDDEN = 2 * NEG
LOG2E = 1.4426950408889634
HEAD = 128


def _fit(size, want, unit=128):
    return max(n for n in range(unit, max(min(want, size), unit) + 1, unit) if size % n == 0)


def _dot(a, b, ca, cb):
    return lax.dot_general(a, b, (((ca,), (cb,)), ((), ())), preferred_element_type=jnp.float32)


def _turn(t, cos, sin, back=False):
    other = pltpu.roll(t, HEAD // 2, 1) * sin
    return t * cos - other if back else t * cos + other


def _blocks(iq, bq, bk, total):
    return lax.div(iq * bq + 1, bk), jnp.minimum(lax.div(iq * bq + bq - 1 + bk, bk), total)


def _gap(bk, bq):
    return lax.broadcasted_iota(jnp.int32, (bk, bq), 1) - lax.broadcasted_iota(jnp.int32, (bk, bq), 0)


def _cols(n):
    return slice(n * HEAD, (n + 1) * HEAD)


def _turn_keys(k_ref, cos_ref, sin_ref, k_s):
    step = 256

    @pl.loop(0, k_ref.shape[0] // step)
    def _(i):
        r = pl.ds(pl.multiple_of(i * step, step), step)
        for n in range(k_ref.shape[1] // HEAD):
            k_s[r, _cols(n)] = _turn(k_ref[r, _cols(n)].astype(jnp.float32), cos_ref[r, :], sin_ref[r, :]).astype(k_s.dtype)


def _turn_queries(iq, q_ref, cos_ref, sin_ref, q_s):
    bq = q_ref.shape[0]
    here = pl.ds(pl.multiple_of(iq * bq, bq), bq)
    for n in range(q_ref.shape[1] // HEAD):
        q_s[:, _cols(n)] = _turn(q_ref[:, _cols(n)].astype(jnp.float32), cos_ref[here, :], sin_ref[here, :]).astype(q_s.dtype)


def _forward(q_ref, k_ref, v_ref, cos_ref, sin_ref, o_ref, lse_ref, q_s, k_s, top_s, mix_s, gap_s, *, bk):
    bq, heads, kv = q_ref.shape[0], q_ref.shape[1] // HEAD, k_ref.shape[1] // HEAD
    g, scale = heads // kv, HEAD**-0.5
    e, low = scale * LOG2E, q_ref.dtype
    iq = pl.program_id(0)

    @pl.when(iq == 0)
    def _():
        gap_s[...] = _gap(bk, bq)
        _turn_keys(k_ref, cos_ref, sin_ref, k_s)

    _turn_queries(iq, q_ref, cos_ref, sin_ref, q_s)
    top_s[...] = jnp.full_like(top_s, NEG)
    mix_s[...] = jnp.zeros_like(mix_s)
    ones = jnp.ones((8, bk), low)

    def block(j, masked):
        here = pl.ds(pl.multiple_of(j * bk, bk), bk)
        scores = [_dot(k_s[here, _cols(n // g)], q_s[:, _cols(n)], 1, 1) for n in range(heads)]
        ok = gap_s[...] >= j * bk - iq * bq if masked else None
        weights, keeps = [], []
        for n, s in enumerate(scores):
            if masked:
                s = jnp.where(ok, s, HIDDEN)
            old = top_s[n : n + 1, :]
            top = jnp.maximum(old, s.max(axis=0, keepdims=True))
            top_s[n : n + 1, :] = top
            weights.append(jnp.exp2((s - top) * e).astype(low))
            keeps.append(jnp.exp2((old - top) * e))
        for n, (p, keep) in enumerate(zip(weights, keeps)):
            values = jnp.concatenate([v_ref[here, _cols(n // g)].T, ones], axis=0)
            mix_s[n] = mix_s[n] * keep + _dot(values, p, 1, 0)

    whole, last = _blocks(iq, bq, bk, k_ref.shape[0] // bk)
    lax.fori_loop(0, whole, lambda j, _: block(j, False), None)
    lax.fori_loop(whole, last, lambda j, _: block(j, True), None)
    for n in range(heads):
        total = mix_s[n, HEAD : HEAD + 1, :]
        o_ref[:, _cols(n)] = (mix_s[n, :HEAD, :] * (1 / total)).T.astype(o_ref.dtype)
        lse_ref[n : n + 1, :] = top_s[n : n + 1, :] * scale + jnp.log(total)


def _backward(q_ref, k_ref, v_ref, cos_ref, sin_ref, do_ref, o_ref, lse_ref, *rest, bk, moved):
    given, rest = rest[:moved], rest[moved:]
    dq_ref, dk_ref, dv_ref = rest[:3]
    taken, (q_s, k_s, dq_s, dk_s, dv_s, gap_s, sem) = rest[3 : 3 + moved], rest[3 + moved :]
    bq, heads, kv = q_ref.shape[0], q_ref.shape[1] // HEAD, k_ref.shape[1] // HEAD
    g, scale = heads // kv, HEAD**-0.5
    e, low = scale * LOG2E, q_ref.dtype
    iq = pl.program_id(0)

    @pl.when(iq == 0)
    def _():
        gap_s[...] = _gap(bk, bq)
        _turn_keys(k_ref, cos_ref, sin_ref, k_s)
        dk_s[...] = jnp.zeros_like(dk_s)
        dv_s[...] = jnp.zeros_like(dv_s)

    _turn_queries(iq, q_ref, cos_ref, sin_ref, q_s)
    dq_s[...] = jnp.zeros_like(dq_s)
    copies = []
    for i, (source, target) in enumerate(zip(given, taken)):
        r, c = source.shape
        here = pl.ds(pl.multiple_of(iq * r, r), r), slice(None)
        if r == target.shape[0]:
            here = slice(None), pl.ds(pl.multiple_of(iq * c, c), c)
        copies.append(pltpu.make_async_copy(source, target.at[here], sem.at[i]))
        copies[-1].start()
    lses, deltas = [], []
    for n in range(heads):
        both = do_ref[:, _cols(n)].astype(jnp.float32) * o_ref[:, _cols(n)].astype(jnp.float32)
        deltas.append(both.T.sum(axis=0, keepdims=True))
        lses.append(lse_ref[n : n + 1, :] * LOG2E)

    def block(j, masked):
        here = pl.ds(pl.multiple_of(j * bk, bk), bk)
        scores = [_dot(k_s[here, _cols(n // g)], q_s[:, _cols(n)], 1, 1) for n in range(heads)]
        dps = [_dot(v_ref[here, _cols(n // g)], do_ref[:, _cols(n)], 1, 1) for n in range(heads)]
        ok = gap_s[...] >= j * bk - iq * bq if masked else None
        for n in range(heads):
            p = jnp.exp2(scores[n] * e - lses[n])
            if masked:
                p = jnp.where(ok, p, 0.0)
            ds = (p * (dps[n] - deltas[n])).astype(low)
            c = _cols(n // g)
            dv_s[here, c] += _dot(p.astype(low), do_ref[:, _cols(n)], 1, 0)
            dk_s[here, c] += _dot(ds, q_s[:, _cols(n)], 1, 0)
            dq_s[n] += _dot(k_s[here, c].T, ds, 1, 0)

    whole, last = _blocks(iq, bq, bk, k_ref.shape[0] // bk)
    lax.fori_loop(0, whole, lambda j, _: block(j, False), None)
    lax.fori_loop(whole, last, lambda j, _: block(j, True), None)
    mine = pl.ds(pl.multiple_of(iq * bq, bq), bq)
    for n in range(heads):
        dq_ref[:, _cols(n)] = _turn((dq_s[n] * scale).T, cos_ref[mine, :], sin_ref[mine, :], True).astype(dq_ref.dtype)

    for copy in copies:
        copy.wait()

    @pl.when(iq == pl.num_programs(0) - 1)
    def _():
        step = 256

        @pl.loop(0, dk_s.shape[0] // step)
        def _(i):
            r = pl.ds(pl.multiple_of(i * step, step), step)
            dv_ref[r, :] = dv_s[r, :].astype(dv_ref.dtype)
            for n in range(kv):
                dk_ref[r, _cols(n)] = _turn(dk_s[r, _cols(n)] * scale, cos_ref[r, :], sin_ref[r, :], True).astype(dk_ref.dtype)


def _views(qkv, width, kv_width, bq):
    tokens = qkv.shape[0]
    at = width // kv_width
    return [pl.BlockSpec((bq, width), lambda i: (i, 0)), pl.BlockSpec((tokens, kv_width), lambda i: (0, at)), pl.BlockSpec((tokens, kv_width), lambda i: (0, at + 1))]


def attention_back(qkv, cos, sin, d_out, out, lse, kv_width, pass_on, *, bq=256, bk=256):
    tokens, width = d_out.shape
    heads = width // HEAD
    bq, bk = _fit(tokens, bq), _fit(tokens, bk)
    steps = tokens // bq
    mine = pl.BlockSpec((bq, width), lambda i: (i, 0))
    table = pl.BlockSpec((tokens, HEAD), lambda i: (0, 0))
    keys = pl.BlockSpec((tokens, kv_width), lambda i: (0, 0))
    runs = [pl.BlockSpec((t.shape[0] // steps, t.shape[1]), lambda i: (i, 0)) if t.shape[0] % (16 * steps) == 0 else pl.BlockSpec((t.shape[0], t.shape[1] // steps), lambda i: (0, i))
            for t in pass_on]
    low = qkv.dtype
    return pl.pallas_call(
        functools.partial(_backward, bk=bk, moved=len(pass_on)), name="attention_back", grid=(steps,),
        in_specs=[*_views(qkv, width, kv_width, bq), table, table, mine, mine, pl.BlockSpec((heads, bq), lambda i: (0, i)), *runs],
        out_specs=[mine, keys, keys, *(pl.BlockSpec(memory_space=pl.ANY) for _ in pass_on)],
        out_shape=[jax.ShapeDtypeStruct((tokens, width), low), jax.ShapeDtypeStruct((tokens, kv_width), low), jax.ShapeDtypeStruct((tokens, kv_width), low),
                   *(jax.ShapeDtypeStruct(t.shape, t.dtype) for t in pass_on)],
        scratch_shapes=[pltpu.VMEM((bq, width), low), pltpu.VMEM((tokens, kv_width), low), pltpu.VMEM((heads, HEAD, bq), jnp.float32),
                        pltpu.VMEM((tokens, kv_width), jnp.float32), pltpu.VMEM((tokens, kv_width), jnp.float32), pltpu.VMEM((bk, bq), jnp.int32),
                        pltpu.SemaphoreType.DMA((max(len(pass_on), 1),))],
        compiler_params=pltpu.CompilerParams(dimension_semantics=("arbitrary",), vmem_limit_bytes=60 * 2**20),
        cost_estimate=pl.CostEstimate(flops=10 * heads * tokens * tokens * HEAD, transcendentals=heads * tokens * tokens, bytes_accessed=8 * tokens * width),
    )(qkv, qkv, qkv, cos, sin, d_out, out, lse, *pass_on)

from jax.sharding import PartitionSpec as P

THETA = 10000
BF16, F32 = jnp.bfloat16, jnp.float32
MESH = pl.DeviceIdType.MESH
ANY = pl.BlockSpec(memory_space=pl.ANY)


def norm_scale(wide):
    return lax.rsqrt(jnp.mean(wide**2, -1, keepdims=True) + 1e-6)


def normed(wide):
    return (wide * norm_scale(wide)).astype(BF16)


def norm_back(wide, by_out):
    scale = norm_scale(wide)
    along = jnp.mean(wide * by_out, -1, keepdims=True)
    return scale * by_out - wide * (along * scale**3)


def tables(tokens, run=128):
    half = HEAD // 2
    pace = float(THETA) ** (-(np.arange(HEAD) % half) / half)
    sign = np.where(np.arange(HEAD) < half, -1.0, 1.0)
    a, b = np.arange(0, tokens, run)[:, None, None] * pace, np.arange(run)[None, :, None] * pace
    ca, sa, cb, sb = (jnp.asarray(t, F32) for t in (np.cos(a), np.sin(a), np.cos(b), np.sin(b)))
    return (ca * cb - sa * sb).reshape(tokens, HEAD), ((sa * cb + ca * sb) * jnp.asarray(sign, F32)).reshape(tokens, HEAD)


class Ring:
    def __init__(self, n, rows):
        self.n, self.rows, self.half = n, rows, rows // 2
        self.me = lax.axis_index("tp")
        self.right, self.left = lax.rem(self.me + 1, n), lax.rem(self.me + n - 1, n)
        self.across = lax.rem(self.me + 2, n)

    def greet(self):
        barrier = pltpu.get_barrier_semaphore()
        for to in (self.left, self.right):
            pl.semaphore_signal(barrier, inc=1, device_id={"tp": to}, device_id_type=MESH)
        pl.semaphore_wait(barrier, 2)

    def copy(self, src, dst, send, recv, to):
        return pltpu.make_async_remote_copy(src_ref=src, dst_ref=dst, send_sem=send, recv_sem=recv, device_id={"tp": to}, device_id_type=MESH)

    def push(self, *where):
        copy = self.copy(*where)
        copy.start()
        return copy

    def places(self, group):
        rows, half = self.rows, self.half
        return {
            "O": (self.me * rows, self.me * rows + half),
            "X": (self.left * rows, self.right * rows + half),
            "Y": (self.left * rows + half, self.right * rows),
            "Z": (self.across * rows, self.across * rows + half),
        }[group]


class Gather:
    def __init__(self, ring, own, at, send, recv, first=None):
        self.ring, self.own, self.send, self.recv, self.copies = ring, own, send, recv, {}
        self.at = dict(at, O=own) if first is None else dict(at, O=own, X=first)

    def step(self, group):
        r, h = self.ring, self.ring.half
        top, bottom = pl.ds(0, h), pl.ds(h, h)
        k = 2 * "XYZ".index(group)
        source = self.at["X" if group == "Z" else "O"]
        right, left = (bottom, top) if group == "Y" else (top, bottom)
        self.copies[group] = (
            r.push(source.at[right], self.at[group].at[top], self.send.at[k], self.recv.at[k], r.right),
            r.push(source.at[left], self.at[group].at[bottom], self.send.at[k + 1], self.recv.at[k + 1], r.left),
        )

    def arrived(self, group):
        for copy in self.copies[group]:
            copy.wait_recv()

    def finish(self):
        for pair in self.copies.values():
            for copy in pair:
                copy.wait_send()

    def rows_of(self, group):
        return self.at[group]


def parts(ref, rows, groups):
    return {group: ref.at[pl.ds(i * rows, rows)] for i, group in enumerate(groups)}


class Scatter:
    def __init__(self, ring, out_s, in_s, send, recv):
        self.ring, self.out, self.inn, self.send, self.recv, self.copies = ring, out_s, in_s, send, recv, {}

    def step(self, group):
        r, h = self.ring, self.ring.half
        k = "XZY".index(group)
        first, second = pl.ds(0, h), pl.ds(h, h)
        right, left = (first, second) if group == "Z" else (second, first)
        lands_r, lands_l = {"X": (second, first), "Z": (second, first), "Y": (first, second)}[group]
        self.copies[group] = (
            r.push(self.out.at[k, right], self.inn.at[k, lands_r], self.send.at[2 * k], self.recv.at[2 * k], r.right),
            r.push(self.out.at[k, left], self.inn.at[k, lands_l], self.send.at[2 * k + 1], self.recv.at[2 * k + 1], r.left),
        )

    def arrived(self, group):
        for copy in self.copies[group]:
            copy.wait_recv()

    def sent(self, group):
        for copy in self.copies[group]:
            copy.wait_send()


def over_rows(rows, step, f):
    @pl.loop(0, rows // step)
    def _(i):
        f(pl.ds(pl.multiple_of(i * step, step), step))


def product(lhs, w, put, *, trans=False, tile):
    @pl.loop(0, w.shape[0 if trans else 1] // tile)
    def _(i):
        c = pl.ds(pl.multiple_of(i * tile, tile), tile)
        put(c, _dot(lhs[...], w[c, :], 1, 1) if trans else _dot(lhs[...], w[:, c], 1, 0))


def over_tokens(a, b, outs, *, tile, wide=None):
    widths = [o.shape[1] for o in outs]
    wide = wide or sum(widths)
    ends = [sum(widths[: i + 1]) for i in range(len(widths))]

    def body(l, r, *targets):
        whole = _dot(l[...], r[...], 0, 0).astype(BF16)
        for target, end in zip(targets, ends):
            target[...] = whole if len(outs) == 1 else whole[:, end - target.shape[1] : end]

    tokens, m = a.shape
    pltpu.emit_pipeline(body, grid=(b.shape[1] // wide, m // tile),
                        in_specs=[pl.BlockSpec((tokens, tile), lambda j, i: (0, i)), pl.BlockSpec((tokens, wide), lambda j, i: (0, j))],
                        out_specs=[pl.BlockSpec((tile, wide if len(outs) == 1 else w), lambda j, i: (i, j)) for w in widths])(a, b, *outs)


def started(*pairs):
    copies = [pltpu.make_async_copy(*p) for p in pairs]
    for c in copies:
        c.start()
    return copies


def ended(copies):
    for c in copies:
        c.wait()


def copy_all(*pairs):
    copies = [pltpu.make_async_copy(*p) for p in pairs]
    for c in copies:
        c.start()
    for c in copies:
        c.wait()


def call(kernel, name, number, count, outs, scratch, flops, size):
    return pl.pallas_call(
        kernel, name=name, in_specs=[ANY] * count, out_specs=[ANY] * len(outs), out_shape=outs, scratch_shapes=scratch,
        compiler_params=pltpu.CompilerParams(collective_id=number, has_side_effects=True, vmem_limit_bytes=60 * 2**20),
        cost_estimate=pl.CostEstimate(flops=flops, bytes_accessed=size, transcendentals=0),
    )


DMA6 = pltpu.SemaphoreType.DMA((6,))
DMA2 = pltpu.SemaphoreType.DMA((2,))


def shape(*dims, dtype=BF16):
    return jax.ShapeDtypeStruct(dims, dtype)


def gather_qkv(n, x, wq, wk, wv):
    rows, d = x.shape
    widths = [t.shape[1] for t in (wq, wk, wv)]
    cols = sum(widths)

    def kernel(x, wq, wk, wv, qkv, a_all, w, lhs, part, send, recv, sem):
        ring = Ring(n, rows)
        h = ring.half
        all_parts = parts(a_all, rows, "OXYZ")
        states = started((x, lhs, sem.at[0]))
        weights = started(*((t, w.at[:, pl.ds(sum(widths[:i]), widths[i])], sem.at[i + 3]) for i, t in enumerate((wq, wk, wv))))
        ring.greet()
        ended(states)

        def norm(r):
            lhs[r] = normed(lhs[r].astype(F32))

        over_rows(rows, 16, norm)
        copy_all((lhs, all_parts["O"], sem.at[0]))
        g = Gather(ring, all_parts["O"], all_parts, send, recv)
        g.step("X")
        g.step("Y")
        ended(weights)
        for group in "OXYZ":
            if group != "O":
                g.arrived(group)
                if group == "X":
                    g.step("Z")
                copy_all((g.rows_of(group), lhs, sem.at[0]))

            def put(c, value):
                part[:, c] = value.astype(BF16)

            product(lhs, w, put, tile=256)
            p0, p1 = ring.places(group)
            copy_all((part.at[pl.ds(0, h)], qkv.at[pl.ds(p0, h)], sem.at[0]), (part.at[pl.ds(h, h)], qkv.at[pl.ds(p1, h)], sem.at[1]))
        g.finish()

    run = call(kernel, "gather_qkv", 1, 4, (shape(n * rows, cols), shape(n * rows, d)),
               [pltpu.VMEM((d, cols), BF16), pltpu.VMEM((rows, d), BF16), pltpu.VMEM((rows, cols), BF16), DMA6, DMA6, DMA6], 2 * n * rows * d * cols, 2 * n * rows * d)
    return run(x, wq, wk, wv)


def attention(n, qkv, cos, sin, kv_width, dy, *, bq=512, bk=256):
    tokens, width = qkv.shape[0], qkv.shape[1] - 2 * kv_width
    heads, (rows, d), low = width // HEAD, dy.shape, qkv.dtype
    bq, bk = _fit(tokens, bq), _fit(tokens, bk)

    def kernel(q_ref, k_ref, v_ref, cos_ref, sin_ref, dy, o_ref, lse_ref, dy_x, q_s, k_s, top_s, mix_s, gap_s, send, recv):
        ring = Ring(n, rows)
        h = ring.half
        top, bottom = pl.ds(0, h), pl.ds(h, h)
        copies = [ring.copy(dy.at[top], dy_x.at[top], send.at[0], recv.at[0], ring.right), ring.copy(dy.at[bottom], dy_x.at[bottom], send.at[1], recv.at[1], ring.left)]

        @pl.when(pl.program_id(0) == 0)
        def _():
            ring.greet()
            for c in copies:
                c.start()

        _forward(q_ref, k_ref, v_ref, cos_ref, sin_ref, o_ref, lse_ref, q_s, k_s, top_s, mix_s, gap_s, bk=bk)

        @pl.when(pl.program_id(0) == pl.num_programs(0) - 1)
        def _():
            for c in copies:
                c.wait()

    table = pl.BlockSpec((tokens, HEAD), lambda i: (0, 0))
    return pl.pallas_call(
        kernel, name="attention", grid=(tokens // bq,), in_specs=[*_views(qkv, width, kv_width, bq), table, table, ANY],
        out_specs=[pl.BlockSpec((bq, width), lambda i: (i, 0)), pl.BlockSpec((heads, bq), lambda i: (0, i)), ANY],
        out_shape=[shape(tokens, width), shape(heads, tokens, dtype=F32), shape(rows, d)],
        scratch_shapes=[pltpu.VMEM((bq, width), low), pltpu.VMEM((tokens, kv_width), low), pltpu.VMEM((heads, bq), F32), pltpu.VMEM((heads, HEAD + 8, bq), F32),
                        pltpu.VMEM((bk, bq), jnp.int32), DMA2, DMA2],
        compiler_params=pltpu.CompilerParams(dimension_semantics=("arbitrary",), collective_id=6, has_side_effects=True, vmem_limit_bytes=60 * 2**20),
        cost_estimate=pl.CostEstimate(flops=4 * heads * tokens * tokens * HEAD, transcendentals=heads * tokens * tokens, bytes_accessed=6 * tokens * width),
    )(qkv, qkv, qkv, cos, sin, dy)


def close(scatter, own, use):
    def f(r):
        use(r, own[r] + scatter.inn[0, r].astype(F32) + scatter.inn[2, r].astype(F32))
    over_rows(scatter.ring.rows, 16, f)


def finish_back(scatter, own, inner, by_out, result, sem):
    scatter.sent("X")
    scatter.sent("Z")
    copy_all((inner, scatter.out.at[0], sem.at[0]), (by_out, scatter.out.at[1], sem.at[1]))
    scatter.arrived("X")
    scatter.arrived("Y")

    def use(r, value):
        scatter.inn[1, r] = (scatter.out[1, r].astype(F32) + norm_back(scatter.out[0, r].astype(F32), value)).astype(BF16)

    close(scatter, own, use)
    copy_all((scatter.inn.at[1], result, sem.at[0]))
    scatter.sent("Y")


def add_came(scatter, term):
    def f(r):
        scatter.out[2, r] = (term[r] + scatter.inn[1, r].astype(F32)).astype(BF16)
    over_rows(scatter.ring.rows, 16, f)


def scatter_out(n, heads, wo, dy, dy_x, w_down, x):
    tokens, width = heads.shape
    rows, d = dy.shape
    hidden = w_down.shape[0]

    def kernel(heads, wo, dy, dy_x, w_down, x, h_out, b_out, grouped, dy_all, dh, w, lhs, wide, total, part, out_s, in_s, send, recv, s_send, s_recv, sem):
        ring = Ring(n, rows)
        h = ring.half
        weights = started((wo, w, sem.at[1]))
        ring.greet()
        sc = Scatter(ring, out_s, in_s, s_send, s_recv)
        all_parts = parts(dy_all, rows, "OXYZ")
        g = Gather(ring, dy, all_parts, send, recv, dy_x)
        g.step("Y")
        ended(weights)

        def term(group, target):
            p0, p1 = ring.places(group)
            at = pl.ds("OXYZ".index(group) * rows, rows)
            copy_all((heads.at[pl.ds(p0, h)], part.at[pl.ds(0, h)], sem.at[0]), (heads.at[pl.ds(p1, h)], part.at[pl.ds(h, h)], sem.at[1]))
            kept = started((part, grouped.at[at], sem.at[0]))
            product(part, w, target, tile=512)
            ended(kept)

        def to_send(k):
            def put(c, value):
                out_s[k, :, c] = value.astype(BF16)
            return put

        def keep(c, value):
            total[:, c] = value

        def hid(group):
            copy_all((g.rows_of(group), lhs, sem.at[0]))
            if group in "OX":
                copy_all((lhs, all_parts[group], sem.at[0]))

            def body(step, w_ref):
                c = pl.ds(pl.multiple_of(step.index[0] * 512, 512), 512)
                wide[:, c] = _dot(lhs[...], w_ref[...], 1, 1).astype(BF16)

            pltpu.emit_pipeline(body, grid=(hidden // 512,), in_specs=[pl.BlockSpec((512, d), lambda j: (j, 0))], _explicit_indices=True)(w_down)
            copy_all((wide, dh.at[pl.ds("OXYZ".index(group) * rows, rows)], sem.at[0]))

        term("X", to_send(0))
        sc.step("X")
        term("Z", to_send(1))
        sc.step("Z")
        g.step("Z")
        term("Y", keep)
        hid("O")
        hid("X")
        g.arrived("Y")
        hid("Y")
        sc.arrived("Z")
        add_came(sc, total)
        sc.step("Y")
        term("O", keep)
        g.arrived("Z")
        hid("Z")
        sc.sent("X")
        sc.sent("Z")
        copy_all((x, lhs, sem.at[0]))
        sc.arrived("X")
        sc.arrived("Y")

        def use(r, value):
            states = (lhs[r].astype(F32) + value).astype(BF16)
            out_s[0, r] = states
            out_s[1, r] = normed(states.astype(F32))

        close(sc, total, use)
        copy_all((out_s.at[0], h_out, sem.at[0]), (out_s.at[1], b_out, sem.at[1]))
        sc.sent("Y")
        g.finish()

    run = call(kernel, "scatter_out", 2, 6, (shape(rows, d), shape(rows, d), shape(tokens, width), shape(tokens, d), shape(tokens, hidden)),
                [pltpu.VMEM((width, d), BF16), pltpu.VMEM((rows, d), BF16), pltpu.VMEM((rows, hidden), BF16), pltpu.VMEM((rows, d), F32), pltpu.VMEM((rows, width), BF16), pltpu.VMEM((3, rows, d), BF16), pltpu.VMEM((3, rows, d), BF16),
                 DMA6, DMA6, DMA6, DMA6, DMA2], 2 * tokens * d * (width + hidden), 2 * tokens * d)
    return run(heads, wo, dy, dy_x, w_down, x)


def feed_forward(n, b, dh, w_gate, w_up, states, dy):
    rows, d = b.shape
    tokens, width = dh.shape
    tile = 512

    def kernel(b, dh, w_gate, w_up, states, dy, by_states, b_all, hidden, d_gate, d_up, by_gate, total, own, out_s, in_s, send, recv, s_send, s_recv, sem):
        ring = Ring(n, rows)
        ring.greet()
        sc = Scatter(ring, out_s, in_s, s_send, s_recv)
        g = Gather(ring, b, parts(b_all, rows, "OXYZ"), send, recv)
        g.step("X")
        g.step("Y")
        copy_all((b, out_s.at[0], sem.at[0]))
        copy_all((out_s.at[0], b_all.at[pl.ds(0, rows)], sem.at[0]))

        def body(acc, ids, b_ref, dh_ref, wg_ref, wu_ref, hid_ref, dg_ref, du_ref):
            gate = lax.dot_general(b_ref[...], wg_ref[...], (((1,), (0,)), ((), ())), preferred_element_type=F32)
            up = lax.dot_general(b_ref[...], wu_ref[...], (((1,), (0,)), ((), ())), preferred_element_type=F32)
            s = 1 / (1 + jnp.exp(-gate))
            silu = gate * s
            by = dh_ref[...].astype(F32)
            hid_ref[...] = (silu * up).astype(BF16)
            dg = (by * up * (s + silu * (1 - s))).astype(BF16)
            du = (by * silu).astype(BF16)
            dg_ref[...] = dg
            du_ref[...] = du

            @pl.when(ids.index[0] == 0)
            def _():
                acc[...] = jnp.zeros_like(acc)

            acc[...] += _dot(dg, wg_ref[...], 1, 1) + _dot(du, wu_ref[...], 1, 1)

        def work(group, acc):
            at = pl.ds("OXYZ".index(group) * rows, rows)
            columns = pl.BlockSpec((rows, tile), lambda j: (0, j))
            weight = pl.BlockSpec((d, tile), lambda j: (0, j))
            pltpu.emit_pipeline(functools.partial(body, acc), grid=(width // tile,), in_specs=[pl.BlockSpec((rows, d), lambda j: (0, 0)), columns, weight, weight],
                                out_specs=[columns] * 3, _explicit_indices=True)(
                g.rows_of(group), dh.at[at], w_gate, w_up, hidden.at[at], d_gate.at[at], d_up.at[at])

        def to_send(k):
            def f(r):
                out_s[k, r] = total[r].astype(BF16)
            over_rows(rows, 16, f)

        work("O", own)
        g.arrived("X")
        g.step("Z")
        work("X", total)
        to_send(0)
        sc.step("X")
        g.arrived("Z")
        work("Z", total)
        to_send(1)
        sc.step("Z")
        g.arrived("Y")
        work("Y", total)
        sc.arrived("Z")
        add_came(sc, total)
        sc.step("Y")
        over_tokens(b_all, d_gate, [by_gate], tile=1024, wide=1024)
        finish_back(sc, own, states, dy, by_states, sem)
        g.finish()

    inner = shape(tokens, width)
    run = call(kernel, "feed_forward", 3, 6, (shape(rows, d), shape(tokens, d), inner, inner, inner, shape(d, width)),
                [pltpu.VMEM((rows, d), F32), pltpu.VMEM((rows, d), F32), pltpu.VMEM((3, rows, d), BF16), pltpu.VMEM((3, rows, d), BF16), DMA6, DMA6, DMA6, DMA6, DMA2],
                12 * tokens * d * width, 6 * d * width)
    return run(b, dh, w_gate, w_up, states, dy)


def gather_heads(n, dh, wo, hidden, dy_all, d_up, b_all):
    rows, d = dh.shape
    width = wo.shape[0]
    inner = hidden.shape[1]

    def kernel(dh, wo, hidden, dy_all, d_up, b_all, d_heads, dh_all, by_down, by_up, w, lhs, part, send, recv, sem):
        ring = Ring(n, rows)
        h = ring.half
        weights = started((wo, w, sem.at[1]))
        ring.greet()
        all_parts = parts(dh_all, rows, "OXYZ")
        g = Gather(ring, dh, all_parts, send, recv)
        g.step("X")
        g.step("Y")
        ended(weights)

        def put(c, value):
            part[:, c] = value.astype(BF16)

        def work(group):
            copy_all((g.rows_of(group), lhs, sem.at[0]))
            if group == "O":
                copy_all((lhs, all_parts["O"], sem.at[0]))
            product(lhs, w, put, trans=True, tile=256)
            p0, p1 = ring.places(group)
            copy_all((part.at[pl.ds(0, h)], d_heads.at[pl.ds(p0, h)], sem.at[0]), (part.at[pl.ds(h, h)], d_heads.at[pl.ds(p1, h)], sem.at[1]))

        work("O")
        over_tokens(hidden, dy_all, [by_down], tile=1024, wide=1024)
        g.arrived("X")
        g.step("Z")
        work("X")
        over_tokens(b_all, d_up, [by_up], tile=1024, wide=1024)
        g.arrived("Y")
        work("Y")
        g.arrived("Z")
        work("Z")
        g.finish()

    run = call(kernel, "gather_heads", 4, 6,
                (shape(n * rows, width), shape(n * rows, d), shape(inner, d), shape(d, inner)),
                [pltpu.VMEM((width, d), BF16), pltpu.VMEM((rows, d), BF16), pltpu.VMEM((rows, width), BF16), DMA6, DMA6, DMA2], 2 * n * rows * d * (width + inner), 2 * n * rows * d)
    return run(dh, wo, hidden, dy_all, d_up, b_all)


def scatter_in(n, dq, dk, dv, wq, wk, wv, heads, dh_all, a_all, x):
    (tokens, q_cols), k_cols, d = dq.shape, dk.shape[1], wq.shape[0]
    rows, cols = tokens // n, q_cols + 2 * k_cols
    width = heads.shape[1]

    def kernel(dq, dk, dv, wq, wk, wv, heads, dh_all, a_all, x, by_x, grouped, by_q, by_k, by_v, by_o, w, total, part, out_s, in_s, s_send, s_recv, sem, w_sem):
        ring = Ring(n, rows)
        h = ring.half
        sc = Scatter(ring, out_s, in_s, s_send, s_recv)
        columns = ((dq, pl.ds(0, q_cols)), (dk, pl.ds(q_cols, k_cols)), (dv, pl.ds(q_cols + k_cols, k_cols)))
        weights = started(*((t, w.at[:, c], w_sem.at[k]) for k, (t, (_, c)) in enumerate(zip((wq, wk, wv), columns))))
        ring.greet()

        def term(group, target):
            p0, p1 = ring.places(group)
            at = pl.ds("OXYZ".index(group) * rows, rows)
            copy_all(*((t.at[pl.ds(p, h)], part.at[pl.ds(i * h, h), c], sem.at[2 * k + i]) for k, (t, c) in enumerate(columns) for i, p in enumerate((p0, p1))))
            kept = started((part, grouped.at[at], sem.at[0]))
            if group == "X":
                ended(weights)
            product(part, w, target, trans=True, tile=512)
            ended(kept)

        def to_send(k):
            def put(c, value):
                out_s[k, :, c] = value.astype(BF16)
            return put

        def keep(c, value):
            total[:, c] = value

        term("X", to_send(0))
        sc.step("X")
        term("Z", to_send(1))
        sc.step("Z")
        term("Y", keep)
        over_tokens(heads, dh_all, [by_o], tile=width, wide=1024)
        sc.arrived("Z")
        add_came(sc, total)
        sc.step("Y")
        term("O", keep)
        over_tokens(a_all, grouped, [by_q, by_k, by_v], tile=512)
        finish_back(sc, total, x, dh_all.at[pl.ds(0, rows)], by_x, sem)

    run = call(kernel, "scatter_in", 5, 10,
                (shape(rows, d), shape(tokens, cols), shape(d, q_cols), shape(d, k_cols), shape(d, k_cols), shape(width, d)),
                [pltpu.VMEM((d, cols), BF16), pltpu.VMEM((rows, d), F32), pltpu.VMEM((rows, cols), BF16), pltpu.VMEM((3, rows, d), BF16), pltpu.VMEM((3, rows, d), BF16), DMA6, DMA6, DMA6, DMA6],
                4 * tokens * d * (cols + width), 2 * tokens * d)
    return run(dq, dk, dv, wq, wk, wv, heads, dh_all, a_all, x)


def solution(mesh):
    n = mesh.shape["tp"]

    def step(x, dy, wq, wk, wv, wo, w_gate, w_up, w_down):
        x, dy = x[0], dy[0]
        tokens = n * x.shape[0]
        qkv, a_all = gather_qkv(n, x, wq, wk, wv)
        cos, sin = tables(tokens)
        kv_width = wk.shape[1]
        out, lse, dy_x = attention(n, qkv, cos, sin, kv_width, dy)
        h, b, heads, dy_all, d_hid = scatter_out(n, out, wo, dy, dy_x, w_down, x)
        dh, b_all, hidden, d_gate, d_up, by_gate = feed_forward(n, b, d_hid, w_gate, w_up, h, dy)
        d_heads, dh_all, by_down, by_up = gather_heads(n, dh, wo, hidden, dy_all, d_up, b_all)
        dq, dk, dv, by_gate, by_up, by_down = attention_back(qkv, cos, sin, d_heads, out, lse, kv_width, (by_gate, by_up, by_down))
        dx, _, by_q, by_k, by_v, by_o = scatter_in(n, dq, dk, dv, wq, wk, wv, heads, dh_all, a_all, x)
        return dx[None], by_q, by_k, by_v, by_o, by_gate, by_up, by_down

    states, by_columns, by_rows = P("dp", "tp", None), P(None, "tp"), P("tp", None)
    weights = (by_columns, by_columns, by_columns, by_rows, by_columns, by_columns, by_rows)
    own = tuple(P("dp", "tp") if spec == by_columns else P(("dp", "tp"), None) for spec in weights)
    return jax.shard_map(step, mesh=mesh, in_specs=(states, states, *weights), out_specs=(states, *own), check_vma=False)
```
